256 devices in a mesh: samp: 32 (over z, y_hi, core), snp: 8 (over y_lo, x).
Axes of the slice: x: 4, y: 4 (y_hi: 2, y_lo: 2; y = y_hi * 2 + y_lo), z: 8, core: 2. Of those that a mesh axis runs over, the one named last changes fastest.
Arguments:
- genotypes: float32 [8192, 8192], P('samp', 'snp'), may hold values from 0 to 2, as said below
- observed: int32 [8192, 8192], P('samp', 'snp'), may hold values from 0 to 1
Outputs:
- relation: float32 [32, 8, 32, 8192], P(None, 'snp', None, 'samp')
The draws below stay inside these ranges and needn't reach their ends.
Inputs may be any that keep to these rules, and one draw needn't show every extreme that they name: `genotypes`: dosages are real numbers between 0 and 2.
All inputs are finite; a program needn't handle non-finite values.
Results may differ from the reference program's by a relative error of at most 0.00061.
Values may be sent and summed in bfloat16 or wider, within the bound.
A program may use at most 128 MiB of HBM per device.

```python
import jax
import jax.numpy as jnp
from jax import lax

SAMPLES = 8192
SNPS = 8192
TILE = 32
N_SAMP = 32
N_SNP = 8


def soft_allele(key, threshold, error_top):
    hard_key = jax.random.fold_in(key, 1)
    error_key = jax.random.fold_in(key, 2)
    carried = jax.random.uniform(hard_key, threshold.shape, jnp.float32) < threshold
    error = jax.random.uniform(error_key, threshold.shape, jnp.float32) * error_top
    return jnp.where(carried, 1.0 - error, error)


def draw_genotypes(key, part):
    rate_key = jax.random.fold_in(key, 11)
    first_key = jax.random.fold_in(key, 12)
    second_key = jax.random.fold_in(key, 13)
    base_rate = jax.random.uniform(rate_key, (SNPS,), jnp.float32, 0.005, 0.331)
    position = (jnp.arange(SAMPLES, dtype=jnp.float32) / SAMPLES)[:, None]
    threshold = base_rate[None, :] * (1.0 + 2.0 * position)
    first_allele = soft_allele(first_key, threshold, 0.3)
    second_allele = soft_allele(second_key, threshold, 0.3)
    return jnp.clip(first_allele + second_allele, 0.0, 2.0).astype(jnp.float32)


def draw_observed(key, part):
    shift_key = jax.random.fold_in(key, 21)
    call_key = jax.random.fold_in(key, 22)
    snp_shift = jax.random.randint(shift_key, (SNPS,), 0, 40)
    sample_index = jnp.arange(SAMPLES, dtype=jnp.int32)
    threshold = 500 + 480 * sample_index[:, None] // SAMPLES - snp_shift[None, :]
    call_draw = jax.random.randint(call_key, (SAMPLES, SNPS), 0, 1000)
    return (call_draw < threshold).astype(jnp.int32)


def setup_inputs(seed: int = 0) -> dict:
    key_of = jax.random.split(jax.random.key(seed), 3)
    return {
        "genotypes": draw_genotypes(jax.random.fold_in(key_of[2], 71), 0),
        "observed": draw_observed(jax.random.fold_in(key_of[2], 71), 0),
    }


var_floor = 0.1

def reference(genotypes, observed):
    present = observed.astype(jnp.float32)
    dosage = genotypes.astype(jnp.float32)
    alt_sum = lax.optimization_barrier(jnp.sum(present * dosage, axis=0))
    call_sum = lax.optimization_barrier(jnp.sum(present, axis=0))
    frequency = alt_sum / (2.0 * jnp.maximum(call_sum, 1.0))
    variance = jnp.maximum(2.0 * frequency * (1.0 - frequency), var_floor)
    scaled = (present * (dosage - 2.0 * frequency) * lax.rsqrt(variance)).astype(jnp.bfloat16)
    widened = scaled.astype(jnp.float32)
    grm = jnp.dot(widened, widened.T, precision=lax.Precision.HIGHEST) / SNPS
    return grm.reshape(N_SAMP, N_SNP, TILE, SAMPLES)
```

```python
import jax
import jax.numpy as jnp
from jax import lax
from jax.experimental import pallas as pl
from jax.experimental.pallas import tpu as pltpu
from jax.sharding import PartitionSpec as P

var_floor = 0.1
MESH = pl.DeviceIdType.MESH
NZ, NX, TILE = 8, 4, 32
ROWS, SNPS = 256, 1024
HALF = 128
UNITS = 16
STEPS = 2 * UNITS
EARLY = 6
LAG = 6
X_SHIFT, Y_SHIFT = 16.0, 14.0
STEPS_PER_OCTAVE = 1024.0

STATS_PEERS = [(dz, da, 0, 0, 0) for dz in range(NZ) for da in range(2) if (dz, da) != (0, 0)]
PEERS = (
    [(0, 0, 1, 0, 0)]
    + STATS_PEERS
    + [(0, 0, 0, 0, dx) for dx in range(1, NX)]
    + [(0, 1, 1, 0, 0)]
    + [(0, da, dc, 1, 0) for da in range(2) for dc in range(2)]
)


def encode(value, shift):
    level = jnp.log2(jnp.abs(value)) * STEPS_PER_OCTAVE + (shift * STEPS_PER_OCTAVE + 0.5)
    level = jnp.maximum(level, 0.25).astype(jnp.int32)
    return jnp.where(value < 0.0, -level, level).astype(jnp.int16)


def decode(code, shift):
    level = code.astype(jnp.int32).astype(jnp.float32)
    size = jnp.exp2(jnp.abs(level) * (1.0 / STEPS_PER_OCTAVE) - shift)
    return jnp.clip(level, -1.0, 1.0) * size


def kernel(
    g_hbm, o_hbm, out_ref,
    g_ref, o_ref, part, part_in, pair, sums_in, total, total_in, stats,
    rows_all, cols_all, acc, coded, coded_in, own, sum_coded, sum_in,
    load_sem, st_s, st_r, col_s, col_r, z_s, z_r, x_s, x_r, y_s, y_r,
):
    samp = lax.axis_index("samp")
    snp = lax.axis_index("snp")
    z = lax.div(samp, 4)
    a = lax.rem(lax.div(samp, 2), 2)
    c = lax.rem(samp, 2)
    yl = lax.div(snp, NX)
    x = lax.rem(snp, NX)

    def peer(dz, da, dc, dyl, dx):
        return (
            lax.rem(z + dz, NZ) * 4 + lax.rem(a + da, 2) * 2 + lax.rem(c + dc, 2),
            lax.rem(yl + dyl, 2) * NX + lax.rem(x + dx, NX),
        )

    def send(src, dst, s_sem, r_sem, to):
        return pltpu.make_async_remote_copy(
            src_ref=src, dst_ref=dst, send_sem=s_sem, recv_sem=r_sem, device_id=to, device_id_type=MESH
        )

    loads = [
        pltpu.make_async_copy(g_hbm, g_ref, load_sem.at[0]),
        pltpu.make_async_copy(o_hbm, o_ref, load_sem.at[1]),
    ]
    for copy in loads:
        copy.start()
    barrier = pltpu.get_barrier_semaphore()
    for p in PEERS:
        pl.semaphore_signal(barrier, inc=1, device_id=peer(*p), device_id_type=MESH)
    for copy in loads:
        copy.wait()

    def count(i, carry):
        alt, call = carry
        present = o_ref[pl.ds(i * 8, 8), :].astype(jnp.float32)
        return alt + present * g_ref[pl.ds(i * 8, 8), :], call + present

    zero = jnp.zeros((8, SNPS), jnp.float32)
    alt8, call8 = lax.fori_loop(0, ROWS // 8, count, (zero, zero))
    part[0:1, :] = jnp.sum(alt8, axis=0, keepdims=True)
    part[1:2, :] = jnp.sum(call8, axis=0, keepdims=True)
    pl.semaphore_wait(barrier, len(PEERS))

    mine = pl.ds(pl.multiple_of(c * 512, 512), 512)
    other = pl.ds(pl.multiple_of((1 - c) * 512, 512), 512)
    partner = peer(0, 0, 1, 0, 0)
    swap = send(part.at[:, other], part_in, st_s.at[0], st_r.at[0], partner)
    swap.start()
    swap.wait()
    pair[...] = part[:, mine] + part_in[...]
    spread = []
    for n, p in enumerate(STATS_PEERS):
        copy = send(pair, sums_in.at[n], st_s.at[1 + n], st_r.at[1 + n], peer(*p))
        copy.start()
        spread.append(copy)
    summed = pair[...]
    for n, copy in enumerate(spread):
        copy.wait_recv()
        summed = summed + sums_in[n]
    total[...] = summed
    back = send(total, total_in, st_s.at[16], st_r.at[16], partner)
    back.start()
    stats[:, mine] = summed
    for copy in spread:
        copy.wait_send()
    back.wait()
    stats[:, other] = total_in[...]

    frequency = stats[0:1, :] / (2.0 * jnp.maximum(stats[1:2, :], 1.0))
    variance = jnp.maximum(2.0 * frequency * (1.0 - frequency), var_floor)
    twice = 2.0 * frequency
    scale = lax.rsqrt(variance)

    def standardize(i, carry):
        r = pl.ds(i * 16, 16)
        value = o_ref[r, :].astype(jnp.float32) * (g_ref[r, :] - twice) * scale
        value = value.astype(jnp.bfloat16)
        rows_all[0, r, :] = value
        cols_all[0, r, :] = value
        return carry

    lax.fori_loop(0, ROWS // 16, standardize, 0)

    def unit(i):
        m = i - 2
        r = lax.div(m, 4)
        hr = lax.div(lax.rem(m, 4), 2)
        back_way = lax.rem(m, 2)
        d = jnp.where(back_way == 1, 7 - r, 1 + r)
        d = jnp.where(i < 2, 0, jnp.where(i >= 14, 4, d))
        hr = jnp.where(i < 2, i, jnp.where(i >= 14, i - 14, hr))
        back_way = jnp.where(i >= 14, i - 14, back_way)
        return d, hr, back_way

    def half(hr):
        return pl.ds(pl.multiple_of(lax.rem(yl + hr, 2) * HALF, HALF), HALF)

    def z_send(target):
        d, hr, back_way = unit(target)
        src = jnp.where(back_way == 1, lax.rem(d + 1, NZ), d - 1)
        to = peer(jnp.where(back_way == 1, NZ - 1, 1), 0, 0, 0, 0)
        return send(rows_all.at[src, half(hr)], rows_all.at[d, half(hr)], z_s.at[target], z_r.at[target], to)

    col_copies = [
        send(cols_all.at[0], cols_all.at[2], col_s.at[1], col_r.at[1], peer(0, 1, 0, 0, 0)),
        send(cols_all.at[0], cols_all.at[1], col_s.at[0], col_r.at[0], partner),
        send(cols_all.at[2], cols_all.at[3], col_s.at[2], col_r.at[2], partner),
    ]
    col_copies[0].start()
    for target in range(2, 6):
        z_send(target).start()
    col_copies[1].start()

    def step_unit(t):
        late = t - 2 * EARLY
        i = jnp.where(t < EARLY, t, jnp.where(t < 2 * EARLY, t - EARLY, EARLY + lax.div(late, 2)))
        u = jnp.where(t < EARLY, 0, jnp.where(t < 2 * EARLY, 1, lax.rem(late, 2)))
        return i, u

    def x_send(t, n):
        return send(coded.at[t, n], coded_in.at[t, n], x_s.at[t, n], x_r.at[t, n], peer(0, 0, 0, 0, n + 1))

    def y_send(t, jj):
        i, u = step_unit(t)
        d, hr, _ = unit(i)
        j = 2 * u + jj
        return send(
            sum_coded.at[t, jj], sum_in.at[d, j, hr], y_s.at[t, jj], y_r.at[d, j, hr], peer(0, u, jj, hr, 0)
        )

    def produce(t):
        i, u = step_unit(t)
        d, hr, _ = unit(i)

        @pl.when(jnp.logical_and(u == 0, i >= 2))
        def _():
            z_send(i).wait_recv()

            @pl.when(i < 10)
            def _():
                z_send(i + 4).start()

            @pl.when(i == 10)
            def _():
                z_send(14).start()

            @pl.when(i == 13)
            def _():
                z_send(15).start()

        lhs = rows_all[d, half(hr), :]
        rhs = cols_all[pl.ds(2 * u, 2), :, :].reshape(512, SNPS)
        acc[...] = lax.dot_general(lhs, rhs, (((1,), (1,)), ((), ())), preferred_element_type=jnp.float32)
        for n in range(NX - 1):
            rows = pl.ds(pl.multiple_of(lax.rem(x + n + 1, NX) * TILE, TILE), TILE)
            coded[t, n] = encode(acc[rows, :], X_SHIFT)
            x_send(t, n).start()
        own[t] = acc[pl.ds(pl.multiple_of(x * TILE, TILE), TILE), :]

    def consume(t):
        i, u = step_unit(t)
        d, hr, _ = unit(i)
        value = own[t]
        for n in range(NX - 1):
            x_send(t, n).wait_recv()
            value = value + decode(coded_in[t, n], X_SHIFT)
        code = encode(value, Y_SHIFT)
        sum_coded[t, 0] = code[:, 0:256]
        sum_coded[t, 1] = code[:, 256:512]
        here = jnp.logical_and(u == 0, hr == 0)

        @pl.when(here)
        def _():
            sum_in[d, 0, 0] = code[:, 0:256]

        @pl.when(jnp.logical_not(here))
        def _():
            y_send(t, 0).start()

        y_send(t, 1).start()

    def step(t, carry):
        @pl.when(t == 0)
        def _():
            col_copies[1].wait_recv()

        @pl.when(t == EARLY)
        def _():
            col_copies[0].wait_recv()
            col_copies[2].start()
            col_copies[2].wait_recv()

        @pl.when(t < STEPS)
        def _():
            produce(t)

        @pl.when(t >= LAG)
        def _():
            consume(t - LAG)

        return carry

    lax.fori_loop(0, STEPS + LAG, step, 0)

    def finish(d, carry):
        for j in range(4):
            if j:
                y_wait(d, j, 0)
            y_wait(d, j, 1)
            value = decode(sum_in[d, j, 0], Y_SHIFT) + decode(sum_in[d, j, 1], Y_SHIFT)
            q = lax.rem(z + NZ - d, NZ) * 4 + lax.rem(a + j // 2, 2) * 2 + lax.rem(c + j % 2, 2)
            out_ref[q, 0] = value * (1.0 / 8192.0)
        return carry

    def y_wait(d, j, hr):
        send(sum_coded.at[0, 0], sum_in.at[d, j, hr], y_s.at[0, 0], y_r.at[d, j, hr], partner).wait_recv()

    lax.fori_loop(0, NZ, finish, 0)

    for copy in col_copies:
        copy.wait_send()

    def drain_z(i, carry):
        z_send(i).wait_send()
        return carry

    lax.fori_loop(2, UNITS, drain_z, 0)

    def drain(t, carry):
        for n in range(NX - 1):
            x_send(t, n).wait_send()
        i, u = step_unit(t)
        _, hr, _ = unit(i)

        @pl.when(jnp.logical_not(jnp.logical_and(u == 0, hr == 0)))
        def _():
            y_send(t, 0).wait_send()

        y_send(t, 1).wait_send()
        return carry

    lax.fori_loop(0, STEPS, drain, 0)


def body(genotypes, observed):
    f32, bf16, s16 = jnp.float32, jnp.bfloat16, jnp.int16
    dma = pltpu.SemaphoreType.DMA
    return pl.pallas_call(
        kernel,
        out_shape=jax.ShapeDtypeStruct((32, 1, TILE, ROWS), f32),
        in_specs=[pl.BlockSpec(memory_space=pl.ANY)] * 2,
        out_specs=pl.BlockSpec(memory_space=pltpu.VMEM),
        scratch_shapes=[
            pltpu.VMEM((ROWS, SNPS), f32),
            pltpu.VMEM((ROWS, SNPS), jnp.int32),
            pltpu.VMEM((2, SNPS), f32),
            pltpu.VMEM((2, 512), f32),
            pltpu.VMEM((2, 512), f32),
            pltpu.VMEM((15, 2, 512), f32),
            pltpu.VMEM((2, 512), f32),
            pltpu.VMEM((2, 512), f32),
            pltpu.VMEM((2, SNPS), f32),
            pltpu.VMEM((NZ, ROWS, SNPS), bf16),
            pltpu.VMEM((4, ROWS, SNPS), bf16),
            pltpu.VMEM((HALF, 512), f32),
            pltpu.VMEM((STEPS, 3, TILE, 512), s16),
            pltpu.VMEM((STEPS, 3, TILE, 512), s16),
            pltpu.VMEM((STEPS, TILE, 512), f32),
            pltpu.VMEM((STEPS, 2, TILE, ROWS), s16),
            pltpu.VMEM((NZ, 4, 2, TILE, ROWS), s16),
            dma((2,)),
            dma((17,)),
            dma((17,)),
            dma((3,)),
            dma((3,)),
            dma((UNITS,)),
            dma((UNITS,)),
            dma((STEPS, 3)),
            dma((STEPS, 3)),
            dma((STEPS, 2)),
            dma((NZ, 4, 2)),
        ],
        compiler_params=pltpu.CompilerParams(
            collective_id=0, has_side_effects=True, vmem_limit_bytes=60 * 2**20
        ),
    )(genotypes, observed)


def solution(mesh):
    return jax.shard_map(
        body,
        mesh=mesh,
        in_specs=(P("samp", "snp"), P("samp", "snp")),
        out_specs=P(None, "snp", None, "samp"),
        check_vma=False,
    )
```

```python
import jax
import jax.numpy as jnp
from jax import lax
from jax.experimental import pallas as pl
from jax.experimental.pallas import tpu as pltpu
from jax.sharding import PartitionSpec as P

var_floor = 0.1
MESH = pl.DeviceIdType.MESH
NZ, NX, TILE = 8, 4, 32
ROWS, SNPS = 256, 1024
HALF = 128
UNITS = 16
STEPS = 2 * UNITS
EARLY = 6
RELAY_LAG, SUM_LAG = 4, 8
X_SHIFT, Y_SHIFT = 15.0, 14.0
STEPS_PER_OCTAVE = 1024.0
LANES = (slice(0, 256), slice(256, 512))
ORDER = (0, 1, 7, 2, 6, 3, 5, 4)
FINISH = (20, 24, 25, 32, 33)

PLANE_PEERS = [(0, 0, 1, 0, 0), (0, 1, 0, 0, 0), (0, 1, 1, 0, 0)]
PEERS = (
    PLANE_PEERS
    + [(dz, 0, 0, 0, 0) for dz in range(1, NZ)]
    + [(0, 0, 0, 0, dx) for dx in range(1, NX)]
    + [(0, da, dc, 1, 0) for da in range(2) for dc in range(2)]
)


def encode(value, shift):
    level = jnp.log2(jnp.abs(value)) * STEPS_PER_OCTAVE + (shift * STEPS_PER_OCTAVE + 0.5)
    level = jnp.maximum(level, 0.25).astype(jnp.int32)
    return jnp.where(value < 0.0, -level, level).astype(jnp.int16)


def decode(code, shift):
    level = code.astype(jnp.int32).astype(jnp.float32)
    size = jnp.exp2(jnp.abs(level) * (1.0 / STEPS_PER_OCTAVE) - shift)
    return jnp.clip(level, -1.0, 1.0) * size


def kernel(
    g_hbm, o_hbm, out_ref,
    g_ref, o_ref, part, part_in, sums, total,
    rows_all, cols_all, acc, coded, relay_in, coded_in, own, kept, sum_coded, sum_in,
    load_sem, pl_s, pl_r, st_s, st_r, col_s, col_r, z_s, z_r, x_s, rel_r, x_r, y_s, y_r,
):
    samp = lax.axis_index("samp")
    snp = lax.axis_index("snp")
    z = lax.div(samp, 4)
    a = lax.rem(lax.div(samp, 2), 2)
    c = lax.rem(samp, 2)
    yl = lax.div(snp, NX)
    x = lax.rem(snp, NX)

    def peer(dz, da, dc, dyl, dx):
        return (
            lax.rem(z + dz, NZ) * 4 + lax.rem(a + da, 2) * 2 + lax.rem(c + dc, 2),
            lax.rem(yl + dyl, 2) * NX + lax.rem(x + dx, NX),
        )

    def send(src, dst, s_sem, r_sem, to):
        return pltpu.make_async_remote_copy(
            src_ref=src, dst_ref=dst, send_sem=s_sem, recv_sem=r_sem, device_id=to, device_id_type=MESH
        )

    loads = [
        pltpu.make_async_copy(g_hbm, g_ref, load_sem.at[0]),
        pltpu.make_async_copy(o_hbm, o_ref, load_sem.at[1]),
    ]
    for copy in loads:
        copy.start()
    barrier = pltpu.get_barrier_semaphore()
    for p in PEERS:
        pl.semaphore_signal(barrier, inc=1, device_id=peer(*p), device_id_type=MESH)
    for copy in loads:
        copy.wait()

    def count(i, carry):
        alt, call = carry
        present = o_ref[pl.ds(i * 8, 8), :].astype(jnp.float32)
        return alt + present * g_ref[pl.ds(i * 8, 8), :], call + present

    zero = jnp.zeros((8, SNPS), jnp.float32)
    alt8, call8 = lax.fori_loop(0, ROWS // 8, count, (zero, zero))
    part[0:1, :] = jnp.sum(alt8, axis=0, keepdims=True)
    part[1:2, :] = jnp.sum(call8, axis=0, keepdims=True)
    pl.semaphore_wait(barrier, len(PEERS))

    partner = peer(0, 0, 1, 0, 0)
    around = [
        send(part, part_in.at[n], pl_s.at[n], pl_r.at[n], peer(*p)) for n, p in enumerate(PLANE_PEERS)
    ]
    for copy in around:
        copy.start()
    for copy in around:
        copy.wait_recv()
    total[...] = (part[...] + part_in[0]) + (part_in[1] + part_in[2])
    along = []
    for dz in range(1, NZ):
        copy = send(total, sums.at[z], st_s.at[dz], st_r.at[z], peer(dz, 0, 0, 0, 0))
        copy.start()
        along.append(copy)
    sums[z] = total[...]
    for dz in range(1, NZ):
        there = lax.rem(z + dz, NZ)
        send(total, sums.at[there], st_s.at[dz], st_r.at[there], partner).wait_recv()
    stats = sums[0]
    for n in range(1, NZ):
        stats = stats + sums[n]

    frequency = stats[0:1, :] / (2.0 * jnp.maximum(stats[1:2, :], 1.0))
    variance = jnp.maximum(2.0 * frequency * (1.0 - frequency), var_floor)
    twice = 2.0 * frequency
    scale = lax.rsqrt(variance)

    def standardize(i, carry):
        r = pl.ds(i * 16, 16)
        value = o_ref[r, :].astype(jnp.float32) * (g_ref[r, :] - twice) * scale
        value = value.astype(jnp.bfloat16)
        rows_all[0, r, :] = value
        cols_all[0, r, :] = value
        return carry

    lax.fori_loop(0, ROWS // 16, standardize, 0)

    def unit(i):
        m = i - 2
        r = lax.div(m, 4)
        hr = lax.div(lax.rem(m, 4), 2)
        back_way = lax.rem(m, 2)
        d = jnp.where(back_way == 1, 7 - r, 1 + r)
        d = jnp.where(i < 2, 0, jnp.where(i >= 14, 4, d))
        hr = jnp.where(i < 2, i, jnp.where(i >= 14, i - 14, hr))
        back_way = jnp.where(i >= 14, i - 14, back_way)
        return d, hr, back_way

    def half(hr):
        return pl.ds(pl.multiple_of(lax.rem(yl + hr, 2) * HALF, HALF), HALF)

    def z_send(target):
        d, hr, back_way = unit(target)
        src = jnp.where(back_way == 1, lax.rem(d + 1, NZ), d - 1)
        to = peer(jnp.where(back_way == 1, NZ - 1, 1), 0, 0, 0, 0)
        return send(rows_all.at[src, half(hr)], rows_all.at[d, half(hr)], z_s.at[target], z_r.at[target], to)

    col_copies = [
        send(cols_all.at[0], cols_all.at[2], col_s.at[1], col_r.at[1], peer(0, 1, 0, 0, 0)),
        send(cols_all.at[0], cols_all.at[1], col_s.at[0], col_r.at[0], partner),
        send(cols_all.at[2], cols_all.at[3], col_s.at[2], col_r.at[2], partner),
    ]
    col_copies[0].start()
    for target in range(2, 6):
        z_send(target).start()
    col_copies[1].start()

    def step_unit(t):
        late = t - 2 * EARLY
        i = jnp.where(t < EARLY, t, jnp.where(t < 2 * EARLY, t - EARLY, EARLY + lax.div(late, 2)))
        u = jnp.where(t < EARLY, 0, jnp.where(t < 2 * EARLY, 1, lax.rem(late, 2)))
        return i, u

    def relay_send(t, way):
        return send(
            coded.at[t, way, 0], relay_in.at[t, way], x_s.at[t, way, 0], rel_r.at[t, way], peer(0, 0, 0, 0, 3 if way else 1)
        )

    def x_send(t, way, late):
        return send(
            coded.at[t, way, 1 + late],
            coded_in.at[t, way, late],
            x_s.at[t, way, 1 + late],
            x_r.at[t, way, late],
            peer(0, 0, 0, 0, 3 if way else 1),
        )

    def y_send(t, jj):
        i, u = step_unit(t)
        d, hr, _ = unit(i)
        j = 2 * u + jj
        return send(
            sum_coded.at[t, jj], sum_in.at[d, j, hr], y_s.at[t, jj], y_r.at[d, j, hr], peer(0, u, jj, hr, 0)
        )

    def produce(t):
        i, u = step_unit(t)
        d, hr, _ = unit(i)

        @pl.when(jnp.logical_and(u == 0, i >= 2))
        def _():
            z_send(i).wait_recv()

            @pl.when(i < 10)
            def _():
                z_send(i + 4).start()

            @pl.when(i == 10)
            def _():
                z_send(14).start()

            @pl.when(i == 13)
            def _():
                z_send(15).start()

        lhs = rows_all[d, half(hr), :]
        rhs = cols_all[pl.ds(2 * u, 2), :, :].reshape(512, SNPS)
        acc[...] = lax.dot_general(lhs, rhs, (((1,), (1,)), ((), ())), preferred_element_type=jnp.float32)
        beyond = tile(2)
        for way in range(2):
            coded[t, way, 0] = encode(acc[beyond, LANES[way]], X_SHIFT)
            relay_send(t, way).start()
        for way in range(2):
            there = tile(3 if way else 1)
            coded[t, way, 1] = encode(acc[there, LANES[1 - way]], X_SHIFT)
            x_send(t, way, 0).start()
            kept[t, way] = acc[there, LANES[way]]
        own[t] = acc[tile(0), :]

    def tile(dx):
        return pl.ds(pl.multiple_of(lax.rem(x + dx, NX) * TILE, TILE), TILE)

    def relay(t):
        for way in range(2):
            relay_send(t, way).wait_recv()
            coded[t, way, 2] = encode(kept[t, way] + decode(relay_in[t, way], X_SHIFT), X_SHIFT)
            x_send(t, way, 1).start()

    def consume(t):
        i, u = step_unit(t)
        d, hr, _ = unit(i)
        for way in range(2):
            for late in range(2):
                x_send(t, way, late).wait_recv()
        left = own[t, :, 0:256] + decode(coded_in[t, 0, 1], X_SHIFT) + decode(coded_in[t, 1, 0], X_SHIFT)
        right = own[t, :, 256:512] + decode(coded_in[t, 0, 0], X_SHIFT) + decode(coded_in[t, 1, 1], X_SHIFT)
        code = encode(left, Y_SHIFT)
        sum_coded[t, 0] = code
        here = jnp.logical_and(u == 0, hr == 0)

        @pl.when(here)
        def _():
            sum_in[d, 0, 0] = code

        @pl.when(jnp.logical_not(here))
        def _():
            y_send(t, 0).start()

        sum_coded[t, 1] = encode(right, Y_SHIFT)
        y_send(t, 1).start()

    def step(t, carry):
        @pl.when(t == 0)
        def _():
            col_copies[1].wait_recv()

        @pl.when(t == EARLY)
        def _():
            col_copies[0].wait_recv()
            col_copies[2].start()
            col_copies[2].wait_recv()

        @pl.when(jnp.logical_and(t >= RELAY_LAG, t < STEPS + RELAY_LAG))
        def _():
            relay(t - RELAY_LAG)

        @pl.when(t >= SUM_LAG)
        def _():
            consume(t - SUM_LAG)

        @pl.when(t < STEPS)
        def _():
            produce(t)

        for n, at in enumerate(FINISH):
            @pl.when(t == at)
            def _(n=n):
                finish(ORDER[n])

        return carry

    def finish(d):
        for j in range(4):
            if j:
                y_wait(d, j, 0)
            y_wait(d, j, 1)
            value = decode(sum_in[d, j, 0], Y_SHIFT) + decode(sum_in[d, j, 1], Y_SHIFT)
            q = lax.rem(z + NZ - d, NZ) * 4 + lax.rem(a + j // 2, 2) * 2 + lax.rem(c + j % 2, 2)
            out_ref[q, 0] = value * (1.0 / 8192.0)

    def y_wait(d, j, hr):
        send(sum_coded.at[0, 0], sum_in.at[d, j, hr], y_s.at[0, 0], y_r.at[d, j, hr], partner).wait_recv()

    lax.fori_loop(0, STEPS + SUM_LAG, step, 0)
    for d in ORDER[len(FINISH):]:
        finish(d)

    for copy in around + along:
        copy.wait_send()
    for copy in col_copies:
        copy.wait_send()

    def drain_z(i, carry):
        z_send(i).wait_send()
        return carry

    lax.fori_loop(2, UNITS, drain_z, 0)

    def drain(t, carry):
        for way in range(2):
            relay_send(t, way).wait_send()
            x_send(t, way, 0).wait_send()
            x_send(t, way, 1).wait_send()
        i, u = step_unit(t)
        _, hr, _ = unit(i)

        @pl.when(jnp.logical_not(jnp.logical_and(u == 0, hr == 0)))
        def _():
            y_send(t, 0).wait_send()

        y_send(t, 1).wait_send()
        return carry

    lax.fori_loop(0, STEPS, drain, 0)


def body(genotypes, observed):
    f32, bf16, s16 = jnp.float32, jnp.bfloat16, jnp.int16
    dma = pltpu.SemaphoreType.DMA
    return pl.pallas_call(
        kernel,
        out_shape=jax.ShapeDtypeStruct((32, 1, TILE, ROWS), f32),
        in_specs=[pl.BlockSpec(memory_space=pl.ANY)] * 2,
        out_specs=pl.BlockSpec(memory_space=pltpu.VMEM),
        scratch_shapes=[
            pltpu.VMEM((ROWS, SNPS), f32),
            pltpu.VMEM((ROWS, SNPS), jnp.int32),
            pltpu.VMEM((2, SNPS), f32),
            pltpu.VMEM((3, 2, SNPS), f32),
            pltpu.VMEM((NZ, 2, SNPS), f32),
            pltpu.VMEM((2, SNPS), f32),
            pltpu.VMEM((NZ, ROWS, SNPS), bf16),
            pltpu.VMEM((4, ROWS, SNPS), bf16),
            pltpu.VMEM((HALF, 512), f32),
            pltpu.VMEM((STEPS, 2, 3, TILE, ROWS), s16),
            pltpu.VMEM((STEPS, 2, TILE, ROWS), s16),
            pltpu.VMEM((STEPS, 2, 2, TILE, ROWS), s16),
            pltpu.VMEM((STEPS, TILE, 512), f32),
            pltpu.VMEM((STEPS, 2, TILE, ROWS), f32),
            pltpu.VMEM((STEPS, 2, TILE, ROWS), s16),
            pltpu.VMEM((NZ, 4, 2, TILE, ROWS), s16),
            dma((2,)),
            dma((3,)),
            dma((3,)),
            dma((NZ,)),
            dma((NZ,)),
            dma((3,)),
            dma((3,)),
            dma((UNITS,)),
            dma((UNITS,)),
            dma((STEPS, 2, 3)),
            dma((STEPS, 2)),
            dma((STEPS, 2, 2)),
            dma((STEPS, 2)),
            dma((NZ, 4, 2)),
        ],
        compiler_params=pltpu.CompilerParams(
            collective_id=0, has_side_effects=True, vmem_limit_bytes=int(32 * 2**20)
        ),
    )(pltpu.with_memory_space_constraint(genotypes, pltpu.HBM), pltpu.with_memory_space_constraint(observed, pltpu.HBM))


def solution(mesh):
    return jax.shard_map(
        body,
        mesh=mesh,
        in_specs=(P("samp", "snp"), P("samp", "snp")),
        out_specs=P(None, "snp", None, "samp"),
        check_vma=False,
    )
```

```python
import jax
import jax.numpy as jnp
from jax import lax
from jax.experimental import pallas as pl
from jax.experimental.pallas import tpu as pltpu
from jax.sharding import PartitionSpec as P

var_floor = 0.1
MESH = pl.DeviceIdType.MESH
NZ, NX, TILE = 8, 4, 32
ROWS, SNPS = 256, 1024
HALF = 128
UNITS = 16
STEPS = 2 * UNITS
EARLY = 6
RELAY_LAG, SUM_LAG = 4, 8
X_SHIFT, Y_SHIFT = 15.0, 14.0
STEPS_PER_OCTAVE = 1024.0
DIRECT = 28
PASS_ON = {
    2: ((2, 6), (3, 7)),
    4: ((4, 8), (5, 9)),
    10: ((6, 10), (7, 11)),
    14: ((8, 12), (9, 13)),
    19: ((10, 14),),
    24: ((13, 15),),
}
CHUNKS = 4
LANES = (slice(0, 256), slice(256, 512))
ORDER = (0, 1, 7, 2, 6, 3, 5, 4)
FINISH = (20, 24, 25, 32, 33)
FORWARD = (3, 3, 4, 5)

STATS_PEERS = [(dz, da, 0, 0, 0) for dz in range(NZ) for da in range(2) if (dz, da) != (0, 0)]
PEERS = (
    [(0, 0, 1, 0, 0)]
    + STATS_PEERS
    + [(0, 0, 0, 0, dx) for dx in range(1, NX)]
    + [(0, 1, 1, 0, 0)]
    + [(0, da, dc, 1, 0) for da in range(2) for dc in range(2)]
)


def encode(value, shift):
    level = jnp.log2(jnp.abs(value)) * STEPS_PER_OCTAVE + (shift * STEPS_PER_OCTAVE + 0.5)
    level = jnp.maximum(level, 0.25).astype(jnp.int32)
    return jnp.where(value < 0.0, -level, level).astype(jnp.int16)


def decode(code, shift):
    level = code.astype(jnp.int32).astype(jnp.float32)
    size = jnp.exp2(jnp.abs(level) * (1.0 / STEPS_PER_OCTAVE) - shift)
    return jnp.clip(level, -1.0, 1.0) * size


def kernel(
    g_hbm, o_hbm, out_ref,
    g_ref, o_ref, part, part_in, pair, sums_in, total, total_in,
    rows_all, cols_all, acc, coded, relay_in, coded_in, own, kept, sum_coded, sum_in,
    load_sem, st_s, st_r, col_s, col_r, z_s, z_r, x_s, rel_r, x_r, y_s, y_r,
):
    samp = lax.axis_index("samp")
    snp = lax.axis_index("snp")
    z = lax.div(samp, 4)
    a = lax.rem(lax.div(samp, 2), 2)
    c = lax.rem(samp, 2)
    yl = lax.div(snp, NX)
    x = lax.rem(snp, NX)

    def peer(dz, da, dc, dyl, dx):
        return (
            lax.rem(z + dz, NZ) * 4 + lax.rem(a + da, 2) * 2 + lax.rem(c + dc, 2),
            lax.rem(yl + dyl, 2) * NX + lax.rem(x + dx, NX),
        )

    def send(src, dst, s_sem, r_sem, to):
        return pltpu.make_async_remote_copy(
            src_ref=src, dst_ref=dst, send_sem=s_sem, recv_sem=r_sem, device_id=to, device_id_type=MESH
        )

    def arrived(ref, sem):
        send(ref, ref, sem, sem, peer(0, 0, 1, 0, 0)).wait_recv()

    def sent(ref, sem):
        send(ref, ref, sem, sem, peer(0, 0, 1, 0, 0)).wait_send()

    loads = [
        pltpu.make_async_copy(g_hbm, g_ref, load_sem.at[0]),
        pltpu.make_async_copy(o_hbm, o_ref, load_sem.at[1]),
    ]
    for copy in loads:
        copy.start()
    barrier = pltpu.get_barrier_semaphore()
    for p in PEERS:
        pl.semaphore_signal(barrier, inc=1, device_id=peer(*p), device_id_type=MESH)
    for copy in loads:
        copy.wait()

    def count(i, carry):
        alt, call = carry
        present = o_ref[pl.ds(i * 8, 8), :].astype(jnp.float32)
        return alt + present * g_ref[pl.ds(i * 8, 8), :], call + present

    zero = jnp.zeros((8, SNPS), jnp.float32)
    alt8, call8 = lax.fori_loop(0, ROWS // 8, count, (zero, zero), unroll=4)
    part[0:1, :] = jnp.sum(alt8, axis=0, keepdims=True)
    part[1:2, :] = jnp.sum(call8, axis=0, keepdims=True)
    pl.semaphore_wait(barrier, len(PEERS))

    partner = peer(0, 0, 1, 0, 0)
    mine = pl.ds(pl.multiple_of(c * 512, 512), 512)
    other = pl.ds(pl.multiple_of((1 - c) * 512, 512), 512)
    swap = send(part.at[:, other], part_in, st_s.at[0], st_r.at[0], partner)
    swap.start()
    swap.wait_recv()
    pair[...] = part[:, mine] + part_in[...]
    spread = []
    for n, p in enumerate(STATS_PEERS):
        copy = send(pair, sums_in.at[n], st_s.at[1], st_r.at[1 + n], peer(*p))
        copy.start()
        spread.append(copy)
    summed = pair[...]
    for n, copy in enumerate(spread):
        copy.wait_recv()
        summed = summed + sums_in[n]
    total[...] = summed
    back = send(total, total_in, st_s.at[2], st_r.at[16], partner)
    back.start()

    def standardize(stats, lanes):
        frequency = stats[0:1, :] / (2.0 * jnp.maximum(stats[1:2, :], 1.0))
        variance = jnp.maximum(2.0 * frequency * (1.0 - frequency), var_floor)
        twice = 2.0 * frequency
        scale = lax.rsqrt(variance)

        def rows_of(i, carry):
            r = pl.ds(i * 32, 32)
            value = o_ref[r, lanes].astype(jnp.float32) * (g_ref[r, lanes] - twice) * scale
            value = value.astype(jnp.bfloat16)
            rows_all[0, r, lanes] = value
            cols_all[0, r, lanes] = value
            return carry

        lax.fori_loop(0, ROWS // 32, rows_of, 0, unroll=True)

    def unit(i):
        m = i - 2
        r = lax.div(m, 4)
        hr = lax.div(lax.rem(m, 4), 2)
        back_way = lax.rem(m, 2)
        d = jnp.where(back_way == 1, 7 - r, 1 + r)
        d = jnp.where(i < 2, 0, jnp.where(i >= 14, 4, d))
        hr = jnp.where(i < 2, i, jnp.where(i >= 14, i - 14, hr))
        back_way = jnp.where(i >= 14, i - 14, back_way)
        return d, hr, back_way

    def half(hr):
        return pl.ds(pl.multiple_of(lax.rem(yl + hr, 2) * HALF, HALF), HALF)

    def z_send(target):
        d, hr, back_way = unit(target)
        src = jnp.where(back_way == 1, lax.rem(d + 1, NZ), d - 1)
        to = peer(jnp.where(back_way == 1, NZ - 1, 1), 0, 0, 0, 0)
        return send(rows_all.at[src, half(hr)], rows_all.at[d, half(hr)], z_s, z_r.at[target], to)

    def first_send(target, lanes):
        hr, to = (target - 2) // 2, peer(1 if target % 2 == 0 else NZ - 1, 0, 0, 0, 0)
        d = 1 if target % 2 == 0 else NZ - 1
        return send(
            rows_all.at[0, half(hr), lanes], rows_all.at[d, half(hr), lanes], z_s, z_r.at[target], to
        )

    def col_send(n, src, dst, to):
        r, lanes = pl.ds((n % 2) * HALF, HALF), mine if n < 2 else other
        return send(cols_all.at[src, r, lanes], cols_all.at[dst, r, lanes], col_s, col_r.at[n + (CHUNKS if dst == 3 else 0)], to)

    far_cols = [col_send(n, 0, 2, peer(0, 1, 0, 0, 0)) for n in range(CHUNKS)]
    forwards = [col_send(n, 2, 3, partner) for n in range(CHUNKS)]
    near_cols = send(cols_all.at[0], cols_all.at[1], col_s, col_r.at[2 * CHUNKS], partner)

    standardize(summed, mine)
    for target in range(2, 6):
        first_send(target, mine).start()
    for copy in far_cols[:2]:
        copy.start()
    back.wait_recv()
    standardize(total_in[...], other)
    for target in range(2, 6):
        first_send(target, other).start()
    near_cols.start()
    for copy in far_cols[2:]:
        copy.start()

    def step_unit(t):
        late = t - 2 * EARLY
        i = jnp.where(t < EARLY, t, jnp.where(t < 2 * EARLY, t - EARLY, EARLY + lax.div(late, 2)))
        u = jnp.where(t < EARLY, 0, jnp.where(t < 2 * EARLY, 1, lax.rem(late, 2)))
        return i, u

    def relay_send(t, way):
        return send(
            coded.at[t, way, 0],
            relay_in.at[t, way],
            x_s,
            rel_r.at[t],
            peer(0, 0, 0, 0, jnp.where(t >= DIRECT, 2, 3 if way else 1)),
        )

    def x_send(t, way, late):
        return send(
            coded.at[t, way, 1 + late],
            coded_in.at[t, way, late],
            x_s,
            x_r.at[t],
            peer(0, 0, 0, 0, 3 if way else 1),
        )

    def y_send(t, jj):
        i, u = step_unit(t)
        d, hr, _ = unit(i)
        j = 2 * u + jj
        return send(
            sum_coded.at[t, jj], sum_in.at[d, 2 * j + hr], y_s, y_r.at[d], peer(0, u, jj, hr, 0)
        )

    def produce(t):
        i, u = step_unit(t)
        d, hr, _ = unit(i)

        @pl.when(jnp.logical_and(u == 0, jnp.logical_or(i >= 14, jnp.logical_or(i == 11, i == 12))))
        def _():
            z_send(i).wait_recv()

        lhs = rows_all[d, half(hr), :]
        rhs = cols_all[pl.ds(2 * u, 2), :, :].reshape(512, SNPS)
        acc[...] = lax.dot_general(lhs, rhs, (((1,), (1,)), ((), ())), preferred_element_type=jnp.float32)
        beyond = tile(2)
        for way in range(2):
            coded[t, way, 0] = encode(acc[beyond, LANES[way]], X_SHIFT)
            relay_send(t, way).start()
        for way in range(2):
            there = tile(3 if way else 1)
            coded[t, way, 1] = encode(acc[there, LANES[1 - way]], X_SHIFT)
            x_send(t, way, 0).start()

            @pl.when(t < DIRECT)
            def _():
                kept[t, way] = acc[there, LANES[way]]

            @pl.when(t >= DIRECT)
            def _():
                coded[t, way, 2] = encode(acc[there, LANES[way]], X_SHIFT)
                x_send(t, way, 1).start()

        own[t] = acc[tile(0), :]

    def tile(dx):
        return pl.ds(pl.multiple_of(lax.rem(x + dx, NX) * TILE, TILE), TILE)

    def relay(t):
        arrived(relay_in.at[t], rel_r.at[t])
        for way in range(2):
            coded[t, way, 2] = encode(kept[t, way] + decode(relay_in[t, way], X_SHIFT), X_SHIFT)
            x_send(t, way, 1).start()

    def consume(t):
        i, u = step_unit(t)
        d, hr, _ = unit(i)
        arrived(coded_in.at[t], x_r.at[t])

        @pl.when(t >= DIRECT)
        def _():
            arrived(relay_in.at[t], rel_r.at[t])
            for way in range(2):
                own[t, :, LANES[way]] = own[t, :, LANES[way]] + decode(relay_in[t, way], X_SHIFT)

        left = own[t, :, 0:256] + decode(coded_in[t, 0, 1], X_SHIFT) + decode(coded_in[t, 1, 0], X_SHIFT)
        right = own[t, :, 256:512] + decode(coded_in[t, 0, 0], X_SHIFT) + decode(coded_in[t, 1, 1], X_SHIFT)
        code = encode(left, Y_SHIFT)
        sum_coded[t, 0] = code
        here = jnp.logical_and(u == 0, hr == 0)

        @pl.when(here)
        def _():
            sum_in[d, 0] = code

        @pl.when(jnp.logical_not(here))
        def _():
            y_send(t, 0).start()

        sum_coded[t, 1] = encode(right, Y_SHIFT)
        y_send(t, 1).start()

    def step(t, carry):
        @pl.when(t == 0)
        def _():
            near_cols.wait_recv()

        for n in range(CHUNKS):

            @pl.when(t == FORWARD[n])
            def _(n=n):
                far_cols[n].wait_recv()
                forwards[n].start()

        @pl.when(t == EARLY)
        def _():
            for copy in forwards:
                copy.wait_recv()

        for at, pairs in PASS_ON.items():

            @pl.when(t == at)
            def _(pairs=pairs):
                for got, target in pairs:
                    z_send(got).wait_recv()
                    z_send(target).start()

        @pl.when(jnp.logical_and(t >= RELAY_LAG, t < DIRECT + RELAY_LAG))
        def _():
            relay(t - RELAY_LAG)

        @pl.when(t >= SUM_LAG)
        def _():
            consume(t - SUM_LAG)

        @pl.when(t < STEPS)
        def _():
            produce(t)

        for n, at in enumerate(FINISH):
            @pl.when(t == at)
            def _(n=n):
                finish(ORDER[n])

        return carry

    def finish(d):
        arrived(sum_in.at[d, pl.ds(1, 7)], y_r.at[d])
        for j in range(4):
            value = decode(sum_in[d, 2 * j], Y_SHIFT) + decode(sum_in[d, 2 * j + 1], Y_SHIFT)
            q = lax.rem(z + NZ - d, NZ) * 4 + lax.rem(a + j // 2, 2) * 2 + lax.rem(c + j % 2, 2)
            out_ref[q, 0] = value * (1.0 / 8192.0)

    lax.fori_loop(0, STEPS + SUM_LAG, step, 0)
    for d in ORDER[len(FINISH):]:
        finish(d)

    sent(sums_in, st_s.at[1])
    swap.wait_send()
    back.wait_send()
    sent(cols_all.at[pl.ds(0, 3)], col_s)
    sent(rows_all.at[pl.ds(0, 7)], z_s)
    sent(coded, x_s)
    sent(sum_coded.at[pl.ds(0, STEPS - NZ // 2)], y_s)


def body(genotypes, observed):
    f32, bf16, s16 = jnp.float32, jnp.bfloat16, jnp.int16
    dma = pltpu.SemaphoreType.DMA
    return pl.pallas_call(
        kernel,
        out_shape=jax.ShapeDtypeStruct((32, 1, TILE, ROWS), f32),
        in_specs=[pl.BlockSpec(memory_space=pl.ANY)] * 2,
        out_specs=pl.BlockSpec(memory_space=pltpu.VMEM),
        scratch_shapes=[
            pltpu.VMEM((ROWS, SNPS), f32),
            pltpu.VMEM((ROWS, SNPS), jnp.int32),
            pltpu.VMEM((2, SNPS), f32),
            pltpu.VMEM((2, 512), f32),
            pltpu.VMEM((2, 512), f32),
            pltpu.VMEM((15, 2, 512), f32),
            pltpu.VMEM((2, 512), f32),
            pltpu.VMEM((2, 512), f32),
            pltpu.VMEM((NZ, ROWS, SNPS), bf16),
            pltpu.VMEM((4, ROWS, SNPS), bf16),
            pltpu.VMEM((HALF, 512), f32),
            pltpu.VMEM((STEPS, 2, 3, TILE, ROWS), s16),
            pltpu.VMEM((STEPS, 2, TILE, ROWS), s16),
            pltpu.VMEM((STEPS, 2, 2, TILE, ROWS), s16),
            pltpu.VMEM((STEPS, TILE, 512), f32),
            pltpu.VMEM((STEPS, 2, TILE, ROWS), f32),
            pltpu.VMEM((STEPS, 2, TILE, ROWS), s16),
            pltpu.VMEM((NZ, 8, TILE, ROWS), s16),
            dma((2,)),
            dma((3,)),
            dma((17,)),
            dma(()),
            dma((2 * CHUNKS + 1,)),
            dma(()),
            dma((UNITS,)),
            dma(()),
            dma((STEPS,)),
            dma((STEPS,)),
            dma(()),
            dma((NZ,)),
        ],
        compiler_params=pltpu.CompilerParams(
            collective_id=0, has_side_effects=True, vmem_limit_bytes=int(32 * 2**20)
        ),
    )(pltpu.with_memory_space_constraint(genotypes, pltpu.HBM), pltpu.with_memory_space_constraint(observed, pltpu.HBM))


def solution(mesh):
    return jax.shard_map(
        body,
        mesh=mesh,
        in_specs=(P("samp", "snp"), P("samp", "snp")),
        out_specs=P(None, "snp", None, "samp"),
        check_vma=False,
    )
```

```python
import jax
import jax.numpy as jnp
from jax import lax
from jax.experimental import pallas as pl
from jax.experimental.pallas import tpu as pltpu
from jax.sharding import PartitionSpec as P

var_floor = 0.1
MESH = pl.DeviceIdType.MESH
NZ, NX, TILE = 8, 4, 32
ROWS, SNPS = 256, 1024
HALF = 128
UNITS = 16
STEPS = UNITS
EARLY = 3
RELAY_LAG, SUM_LAG = 2, 4
X_SHIFT, Y_SHIFT = 15.0, 14.0
STEPS_PER_OCTAVE = 1024.0
DIRECT = 15
PASS_ON = {
    1: ((2, 6), (3, 7)),
    2: ((4, 8), (5, 9)),
    6: ((6, 10), (7, 11)),
    8: ((8, 12), (9, 13)),
    10: ((10, 14),),
    12: ((13, 15),),
}
CHUNKS = 4
FORWARD = {2: (0, 1), 3: (2, 3)}
LANES = (slice(0, 256), slice(256, 512))
FINISH = {SUM_LAG + 5: (0,), SUM_LAG + 8: (1, 7), SUM_LAG + 12: (2, 6)}
LAST = (3, 5, 4)

STATS_PEERS = [(dz, da, 0, 0, 0) for dz in range(NZ) for da in range(2) if (dz, da) != (0, 0)]
PEERS = (
    [(0, 0, 1, 0, 0)]
    + STATS_PEERS
    + [(0, 0, 0, 0, dx) for dx in range(1, NX)]
    + [(0, 1, 1, 0, 0)]
    + [(0, da, dc, 1, 0) for da in range(2) for dc in range(2)]
)


def encode(value, shift):
    level = jnp.log2(jnp.abs(value)) * STEPS_PER_OCTAVE + (shift * STEPS_PER_OCTAVE + 0.5)
    level = jnp.maximum(level, 0.25).astype(jnp.int32)
    return jnp.where(value < 0.0, -level, level).astype(jnp.int16)


def decode(code, shift):
    level = code.astype(jnp.int32).astype(jnp.float32)
    size = jnp.exp2(jnp.abs(level) * (1.0 / STEPS_PER_OCTAVE) - shift)
    return jnp.clip(level, -1.0, 1.0) * size


def kernel(
    g_hbm, o_hbm, out_ref,
    g_ref, o_ref, part, part_in, pair, sums_in, total, total_in,
    rows_all, cols_all, acc, coded, relay_in, coded_in, own, kept, sum_coded, sum_in,
    load_sem, st_s, st_r, col_s, col_r, z_s, z_r, x_s, rel_r, x_r, y_s, y_r,
):
    samp = lax.axis_index("samp")
    snp = lax.axis_index("snp")
    z = lax.div(samp, 4)
    a = lax.rem(lax.div(samp, 2), 2)
    c = lax.rem(samp, 2)
    yl = lax.div(snp, NX)
    x = lax.rem(snp, NX)

    def peer(dz, da, dc, dyl, dx):
        return (
            lax.rem(z + dz, NZ) * 4 + lax.rem(a + da, 2) * 2 + lax.rem(c + dc, 2),
            lax.rem(yl + dyl, 2) * NX + lax.rem(x + dx, NX),
        )

    def send(src, dst, s_sem, r_sem, to):
        return pltpu.make_async_remote_copy(
            src_ref=src, dst_ref=dst, send_sem=s_sem, recv_sem=r_sem, device_id=to, device_id_type=MESH
        )

    def arrived(ref, sem):
        send(ref, ref, sem, sem, peer(0, 0, 1, 0, 0)).wait_recv()

    def sent(ref, sem):
        send(ref, ref, sem, sem, peer(0, 0, 1, 0, 0)).wait_send()

    loads = [
        pltpu.make_async_copy(g_hbm, g_ref, load_sem.at[0]),
        pltpu.make_async_copy(o_hbm, o_ref, load_sem.at[1]),
    ]
    for copy in loads:
        copy.start()
    barrier = pltpu.get_barrier_semaphore()
    for p in PEERS:
        pl.semaphore_signal(barrier, inc=1, device_id=peer(*p), device_id_type=MESH)
    for copy in loads:
        copy.wait()

    def count(i, carry):
        alt, call = carry
        present = o_ref[pl.ds(i * 8, 8), :].astype(jnp.float32)
        return alt + present * g_ref[pl.ds(i * 8, 8), :], call + present

    zero = jnp.zeros((8, SNPS), jnp.float32)
    alt8, call8 = lax.fori_loop(0, ROWS // 8, count, (zero, zero), unroll=4)
    part[0:1, :] = jnp.sum(alt8, axis=0, keepdims=True)
    part[1:2, :] = jnp.sum(call8, axis=0, keepdims=True)
    pl.semaphore_wait(barrier, len(PEERS))

    partner = peer(0, 0, 1, 0, 0)
    mine = pl.ds(pl.multiple_of(c * 512, 512), 512)
    other = pl.ds(pl.multiple_of((1 - c) * 512, 512), 512)
    swap = send(part.at[:, other], part_in, st_s.at[0], st_r.at[0], partner)
    swap.start()
    swap.wait_recv()
    pair[...] = part[:, mine] + part_in[...]
    spread = []
    for n, p in enumerate(STATS_PEERS):
        copy = send(pair, sums_in.at[n], st_s.at[1], st_r.at[1 + n], peer(*p))
        copy.start()
        spread.append(copy)
    summed = pair[...]
    for n, copy in enumerate(spread):
        copy.wait_recv()
        summed = summed + sums_in[n]
    total[...] = summed
    back = send(total, total_in, st_s.at[2], st_r.at[16], partner)
    back.start()

    def standardize(stats, lanes):
        frequency = stats[0:1, :] / (2.0 * jnp.maximum(stats[1:2, :], 1.0))
        variance = jnp.maximum(2.0 * frequency * (1.0 - frequency), var_floor)
        twice = 2.0 * frequency
        scale = lax.rsqrt(variance)

        def rows_of(i, carry):
            r = pl.ds(i * 32, 32)
            value = o_ref[r, lanes].astype(jnp.float32) * (g_ref[r, lanes] - twice) * scale
            value = value.astype(jnp.bfloat16)
            rows_all[0, r, lanes] = value
            cols_all[0, r, lanes] = value
            return carry

        lax.fori_loop(0, ROWS // 32, rows_of, 0, unroll=True)

    def unit(i):
        m = i - 2
        r = lax.div(m, 4)
        hr = lax.div(lax.rem(m, 4), 2)
        back_way = lax.rem(m, 2)
        d = jnp.where(back_way == 1, 7 - r, 1 + r)
        d = jnp.where(i < 2, 0, jnp.where(i >= 14, 4, d))
        hr = jnp.where(i < 2, i, jnp.where(i >= 14, i - 14, hr))
        back_way = jnp.where(i >= 14, i - 14, back_way)
        return d, hr, back_way

    def half(hr):
        return pl.ds(pl.multiple_of(lax.rem(yl + hr, 2) * HALF, HALF), HALF)

    def z_send(target):
        d, hr, back_way = unit(target)
        src = jnp.where(back_way == 1, lax.rem(d + 1, NZ), d - 1)
        to = peer(jnp.where(back_way == 1, NZ - 1, 1), 0, 0, 0, 0)
        return send(rows_all.at[src, half(hr)], rows_all.at[d, half(hr)], z_s, z_r.at[target], to)

    def first_send(target, lanes):
        hr, to = (target - 2) // 2, peer(1 if target % 2 == 0 else NZ - 1, 0, 0, 0, 0)
        d = 1 if target % 2 == 0 else NZ - 1
        return send(
            rows_all.at[0, half(hr), lanes], rows_all.at[d, half(hr), lanes], z_s, z_r.at[target], to
        )

    def col_send(n, src, dst, to):
        r, lanes = pl.ds((n % 2) * HALF, HALF), mine if n < 2 else other
        return send(cols_all.at[src, r, lanes], cols_all.at[dst, r, lanes], col_s, col_r.at[n + (CHUNKS if dst == 3 else 0)], to)

    far_cols = [col_send(n, 0, 2, peer(0, 1, 0, 0, 0)) for n in range(CHUNKS)]
    forwards = [col_send(n, 2, 3, partner) for n in range(CHUNKS)]
    near_cols = send(cols_all.at[0], cols_all.at[1], col_s, col_r.at[2 * CHUNKS], partner)

    standardize(summed, mine)
    for target in range(2, 6):
        first_send(target, mine).start()
    for copy in far_cols[:2]:
        copy.start()
    back.wait_recv()
    standardize(total_in[...], other)
    for target in range(2, 6):
        first_send(target, other).start()
    near_cols.start()
    for copy in far_cols[2:]:
        copy.start()

    def step_unit(t):
        late = t - 2 * EARLY
        i = jnp.where(t < EARLY, t, jnp.where(t < 2 * EARLY, t - EARLY, EARLY + lax.div(late, 2)))
        u = jnp.where(t < EARLY, 0, jnp.where(t < 2 * EARLY, 1, lax.rem(late, 2)))
        return 2 * i, u

    def relay_send(t, way):
        return send(
            coded.at[t, way, 0],
            relay_in.at[t, way],
            x_s,
            rel_r.at[t],
            peer(0, 0, 0, 0, jnp.where(t >= DIRECT, 2, 3 if way else 1)),
        )

    def x_send(t, way, late):
        return send(
            coded.at[t, way, 1 + late],
            coded_in.at[t, way, late],
            x_s,
            x_r.at[t],
            peer(0, 0, 0, 0, 3 if way else 1),
        )

    def y_send(t, e, jj):
        i, u = step_unit(t)
        d, hr, _ = unit(i + e)
        return send(
            sum_coded.at[t, jj, pl.ds(e * TILE, TILE)],
            sum_in.at[d, 2 * (2 * u + jj) + hr],
            y_s,
            y_r.at[d],
            peer(0, u, jj, hr, 0),
        )

    def produce(t):
        i, u = step_unit(t)
        d0, hr0, _ = unit(i)
        d1, hr1, _ = unit(i + 1)
        first = u == 0

        @pl.when(jnp.logical_and(first, jnp.logical_or(i == 12, i == 14)))
        def _():
            z_send(i).wait_recv()

        @pl.when(jnp.logical_and(first, jnp.logical_or(i == 10, i == 14)))
        def _():
            z_send(i + 1).wait_recv()

        lhs = jnp.concatenate([rows_all[d0, half(hr0), :], rows_all[d1, half(hr1), :]], axis=0)
        rhs = cols_all[pl.ds(2 * u, 2), :, :].reshape(512, SNPS)
        acc[...] = lax.dot_general(lhs, rhs, (((1,), (1,)), ((), ())), preferred_element_type=jnp.float32)
        for way in range(2):
            for e in range(2):
                coded[t, way, 0, rows(e)] = encode(acc[tile(e, 2), LANES[way]], X_SHIFT)
            relay_send(t, way).start()
        for way in range(2):
            for e in range(2):
                coded[t, way, 1, rows(e)] = encode(acc[tile(e, 3 if way else 1), LANES[1 - way]], X_SHIFT)
            x_send(t, way, 0).start()

        @pl.when(t < DIRECT)
        def _():
            for way in range(2):
                for e in range(2):
                    kept[t, way, rows(e)] = acc[tile(e, 3 if way else 1), LANES[way]]

        @pl.when(t >= DIRECT)
        def _():
            for way in range(2):
                for e in range(2):
                    coded[t, way, 2, rows(e)] = encode(acc[tile(e, 3 if way else 1), LANES[way]], X_SHIFT)
                x_send(t, way, 1).start()

        for e in range(2):
            own[t, rows(e)] = acc[tile(e, 0), :]

    def rows(e):
        return pl.ds(e * TILE, TILE)

    def tile(e, dx):
        return pl.ds(pl.multiple_of(e * HALF + lax.rem(x + dx, NX) * TILE, TILE), TILE)

    def relay(t):
        arrived(relay_in.at[t], rel_r.at[t])
        for way in range(2):
            coded[t, way, 2] = encode(kept[t, way] + decode(relay_in[t, way], X_SHIFT), X_SHIFT)
            x_send(t, way, 1).start()

    def consume(t):
        i, u = step_unit(t)
        arrived(coded_in.at[t], x_r.at[t])

        @pl.when(t >= DIRECT)
        def _():
            arrived(relay_in.at[t], rel_r.at[t])
            for way in range(2):
                own[t, :, LANES[way]] = own[t, :, LANES[way]] + decode(relay_in[t, way], X_SHIFT)

        left = own[t, :, 0:256] + decode(coded_in[t, 0, 1], X_SHIFT) + decode(coded_in[t, 1, 0], X_SHIFT)
        code = encode(left, Y_SHIFT)
        sum_coded[t, 0] = code
        for e in range(2):
            d, hr, _ = unit(i + e)
            here = jnp.logical_and(u == 0, hr == 0)

            @pl.when(here)
            def _(d=d, e=e):
                sum_in[d, 0] = code[e * TILE : (e + 1) * TILE]

            @pl.when(jnp.logical_not(here))
            def _(e=e):
                y_send(t, e, 0).start()

        right = own[t, :, 256:512] + decode(coded_in[t, 0, 0], X_SHIFT) + decode(coded_in[t, 1, 1], X_SHIFT)
        sum_coded[t, 1] = encode(right, Y_SHIFT)
        for e in range(2):
            y_send(t, e, 1).start()

    def step(t, carry):
        @pl.when(t == 0)
        def _():
            near_cols.wait_recv()

        for at, chunks in FORWARD.items():

            @pl.when(t == at)
            def _(chunks=chunks):
                for n in chunks:
                    far_cols[n].wait_recv()
                    forwards[n].start()

        @pl.when(jnp.logical_and(t >= RELAY_LAG, t < DIRECT + RELAY_LAG))
        def _():
            relay(t - RELAY_LAG)

        @pl.when(t >= SUM_LAG)
        def _():
            consume(t - SUM_LAG)

        for at, pairs in PASS_ON.items():

            @pl.when(t == at)
            def _(pairs=pairs):
                for got, target in pairs:
                    z_send(got).wait_recv()
                    z_send(target).start()

        @pl.when(t == EARLY)
        def _():
            for copy in forwards:
                copy.wait_recv()

        @pl.when(t < STEPS)
        def _():
            produce(t)

        for at, planes in FINISH.items():

            @pl.when(t == at)
            def _(planes=planes):
                for d in planes:
                    finish(d)

        return carry

    def finish(d):
        arrived(sum_in.at[d, pl.ds(1, 7)], y_r.at[d])
        for j in range(4):
            value = decode(sum_in[d, 2 * j], Y_SHIFT) + decode(sum_in[d, 2 * j + 1], Y_SHIFT)
            q = lax.rem(z + NZ - d, NZ) * 4 + lax.rem(a + j // 2, 2) * 2 + lax.rem(c + j % 2, 2)
            out_ref[q, 0] = value * (1.0 / 8192.0)

    lax.fori_loop(0, STEPS + SUM_LAG, step, 0)
    for d in LAST:
        finish(d)

    sent(sums_in, st_s.at[1])
    swap.wait_send()
    back.wait_send()
    sent(cols_all.at[pl.ds(0, 3)], col_s)
    sent(rows_all.at[pl.ds(0, 7)], z_s)
    sent(coded, x_s)
    sent(sum_coded.at[pl.ds(0, STEPS - NZ // 4)], y_s)


def body(genotypes, observed):
    f32, bf16, s16 = jnp.float32, jnp.bfloat16, jnp.int16
    dma = pltpu.SemaphoreType.DMA
    return pl.pallas_call(
        kernel,
        out_shape=jax.ShapeDtypeStruct((32, 1, TILE, ROWS), f32),
        in_specs=[pl.BlockSpec(memory_space=pl.ANY)] * 2,
        out_specs=pl.BlockSpec(memory_space=pltpu.VMEM),
        scratch_shapes=[
            pltpu.VMEM((ROWS, SNPS), f32),
            pltpu.VMEM((ROWS, SNPS), jnp.int32),
            pltpu.VMEM((2, SNPS), f32),
            pltpu.VMEM((2, 512), f32),
            pltpu.VMEM((2, 512), f32),
            pltpu.VMEM((15, 2, 512), f32),
            pltpu.VMEM((2, 512), f32),
            pltpu.VMEM((2, 512), f32),
            pltpu.VMEM((NZ, ROWS, SNPS), bf16),
            pltpu.VMEM((4, ROWS, SNPS), bf16),
            pltpu.VMEM((2 * HALF, 512), f32),
            pltpu.VMEM((STEPS, 2, 3, 2 * TILE, ROWS), s16),
            pltpu.VMEM((STEPS, 2, 2 * TILE, ROWS), s16),
            pltpu.VMEM((STEPS, 2, 2, 2 * TILE, ROWS), s16),
            pltpu.VMEM((STEPS, 2 * TILE, 512), f32),
            pltpu.VMEM((STEPS, 2, 2 * TILE, ROWS), f32),
            pltpu.VMEM((STEPS, 2, 2 * TILE, ROWS), s16),
            pltpu.VMEM((NZ, 8, TILE, ROWS), s16),
            dma((2,)),
            dma((3,)),
            dma((17,)),
            dma(()),
            dma((2 * CHUNKS + 1,)),
            dma(()),
            dma((UNITS,)),
            dma(()),
            dma((STEPS,)),
            dma((STEPS,)),
            dma(()),
            dma((NZ,)),
        ],
        compiler_params=pltpu.CompilerParams(
            collective_id=0, has_side_effects=True, vmem_limit_bytes=int(32 * 2**20)
        ),
    )(pltpu.with_memory_space_constraint(genotypes, pltpu.HBM), pltpu.with_memory_space_constraint(observed, pltpu.HBM))


def solution(mesh):
    return jax.shard_map(
        body,
        mesh=mesh,
        in_specs=(P("samp", "snp"), P("samp", "snp")),
        out_specs=P(None, "snp", None, "samp"),
        check_vma=False,
    )
```

```python
import jax
import jax.numpy as jnp
from jax import lax
from jax.experimental import pallas as pl
from jax.experimental.pallas import tpu as pltpu
from jax.sharding import PartitionSpec as P

var_floor = 0.1
MESH = pl.DeviceIdType.MESH
NZ, NX, TILE = 8, 4, 32
ROWS, SNPS = 256, 1024
HALF = 128
UNITS = 16
STEPS = UNITS
EARLY = 3
RELAY_LAG, SUM_LAG = 2, 4
X_SHIFT, Y_SHIFT = 15.0, 14.0
STEPS_PER_OCTAVE = 1024.0
DIRECT = 15
PASS_ON = {
    1: ((2, 6), (3, 7)),
    2: ((4, 8), (5, 9)),
    6: ((6, 10), (7, 11)),
    8: ((8, 12), (9, 13)),
    10: ((10, 14), (11, 15)),
}
CHUNKS = 4
FORWARD = {2: (0, 1), 3: (2, 3)}
LANES = (slice(0, 256), slice(256, 512))
FINISH = {SUM_LAG + 5: (0,), SUM_LAG + 8: (1, 7), SUM_LAG + 12: (2, 6)}
LAST = (3, 5, 4)

STATS_PEERS = sorted(
    [(dz, da, 0, 0, 0) for dz in range(NZ) for da in range(2) if (dz, da) != (0, 0)],
    key=lambda p: (-min(p[0], NZ - p[0]) - 2 * p[1], p),
)
PEERS = (
    STATS_PEERS
    + [(0, 1, 1, 0, 0)]
    + [(0, da, dc, 1, 0) for da in range(2) for dc in range(2)]
    + [(0, 0, 0, 0, dx) for dx in (2, 1, 3)]
    + [(0, 0, 1, 0, 0)]
)


def encode(value, shift):
    level = jnp.log2(jnp.abs(value)) * STEPS_PER_OCTAVE + (shift * STEPS_PER_OCTAVE + 0.5)
    level = jnp.maximum(level, 0.25).astype(jnp.int32)
    return jnp.where(value < 0.0, -level, level).astype(jnp.int16)


def decode(code, shift):
    level = code.astype(jnp.int32).astype(jnp.float32)
    size = jnp.exp2(jnp.abs(level) * (1.0 / STEPS_PER_OCTAVE) - shift)
    return jnp.clip(level, -1.0, 1.0) * size


def kernel(
    g_hbm, o_hbm, out_ref,
    g_ref, o_ref, part, part_in, pair, sums_in, total, total_in,
    rows_all, cols_all, acc, coded, relay_in, coded_in, own, kept, sum_coded, sum_in,
    load_sem, st_s, st_r, col_s, col_r, z_s, z_r, x_s, rel_r, x_r, y_s, y_r,
):
    samp = lax.axis_index("samp")
    snp = lax.axis_index("snp")
    z = lax.div(samp, 4)
    a = lax.rem(lax.div(samp, 2), 2)
    c = lax.rem(samp, 2)
    yl = lax.div(snp, NX)
    x = lax.rem(snp, NX)

    def peer(dz, da, dc, dyl, dx):
        return (
            lax.rem(z + dz, NZ) * 4 + lax.rem(a + da, 2) * 2 + lax.rem(c + dc, 2),
            lax.rem(yl + dyl, 2) * NX + lax.rem(x + dx, NX),
        )

    def send(src, dst, s_sem, r_sem, to):
        return pltpu.make_async_remote_copy(
            src_ref=src, dst_ref=dst, send_sem=s_sem, recv_sem=r_sem, device_id=to, device_id_type=MESH
        )

    def arrived(ref, sem):
        send(ref, ref, sem, sem, peer(0, 0, 1, 0, 0)).wait_recv()

    def sent(ref, sem):
        send(ref, ref, sem, sem, peer(0, 0, 1, 0, 0)).wait_send()

    loads = []
    for n in range(2):
        r = pl.ds(n * HALF, HALF)
        loads.append(pltpu.make_async_copy(g_hbm.at[r], g_ref.at[r], load_sem.at[2 * n]))
        loads.append(pltpu.make_async_copy(o_hbm.at[r], o_ref.at[r], load_sem.at[2 * n + 1]))
    for copy in loads:
        copy.start()
    barrier = pltpu.get_barrier_semaphore()
    for p in PEERS:
        pl.semaphore_signal(barrier, inc=1, device_id=peer(*p), device_id_type=MESH)
    def count(i, carry):
        alt, call = carry
        present = o_ref[pl.ds(i * 8, 8), :].astype(jnp.float32)
        return alt + present * g_ref[pl.ds(i * 8, 8), :], call + present

    zero = jnp.zeros((8, SNPS), jnp.float32)
    counts = (zero, zero)
    for n in range(2):
        for copy in loads[2 * n : 2 * n + 2]:
            copy.wait()
        counts = lax.fori_loop(n * HALF // 8, (n + 1) * HALF // 8, count, counts, unroll=8)
    alt8, call8 = counts
    part[0:1, :] = jnp.sum(alt8, axis=0, keepdims=True)
    part[1:2, :] = jnp.sum(call8, axis=0, keepdims=True)
    pl.semaphore_wait(barrier, len(PEERS))

    partner = peer(0, 0, 1, 0, 0)
    mine = pl.ds(pl.multiple_of(c * 512, 512), 512)
    other = pl.ds(pl.multiple_of((1 - c) * 512, 512), 512)
    swap = send(part.at[:, other], part_in, st_s.at[0], st_r.at[0], partner)
    swap.start()
    swap.wait_recv()
    pair[...] = part[:, mine] + part_in[...]
    spread = []
    for n, p in enumerate(STATS_PEERS):
        copy = send(pair, sums_in.at[n], st_s.at[1], st_r.at[1 + n], peer(*p))
        copy.start()
        spread.append(copy)
    summed = pair[...]
    for n, copy in reversed(list(enumerate(spread))):
        copy.wait_recv()
        summed = summed + sums_in[n]
    total[...] = summed
    back = send(total, total_in, st_s.at[2], st_r.at[16], partner)
    back.start()

    def standardize(stats, lanes):
        frequency = stats[0:1, :] / (2.0 * jnp.maximum(stats[1:2, :], 1.0))
        variance = jnp.maximum(2.0 * frequency * (1.0 - frequency), var_floor)
        twice = 2.0 * frequency
        scale = lax.rsqrt(variance)

        def rows_of(i, carry):
            r = pl.ds(i * 32, 32)
            value = o_ref[r, lanes].astype(jnp.float32) * (g_ref[r, lanes] - twice) * scale
            value = value.astype(jnp.bfloat16)
            rows_all[0, r, lanes] = value
            cols_all[0, r, lanes] = value
            return carry

        lax.fori_loop(0, ROWS // 32, rows_of, 0, unroll=True)

    def unit(i):
        m = i - 2
        r = lax.div(m, 4)
        back_way = lax.rem(m, 2)
        hr = lax.rem(lax.div(lax.rem(m, 4), 2) + back_way, 2)
        d = jnp.where(back_way == 1, 7 - r, 1 + r)
        d = jnp.where(i < 2, 0, jnp.where(i >= 14, 4, d))
        hr = jnp.where(i < 2, i, jnp.where(i >= 14, i - 14, hr))
        back_way = jnp.where(i >= 14, i - 14, back_way)
        return d, hr, back_way

    def half(hr):
        return pl.ds(pl.multiple_of(lax.rem(yl + hr, 2) * HALF, HALF), HALF)

    def z_send(target):
        d, hr, back_way = unit(target)
        src = jnp.where(back_way == 1, lax.rem(d + 1, NZ), d - 1)
        to = peer(jnp.where(back_way == 1, NZ - 1, 1), 0, 0, 0, 0)
        return send(rows_all.at[src, half(hr)], rows_all.at[d, half(hr)], z_s, z_r.at[target], to)

    def first_send(target, lanes):
        hr, to = ((target - 2) // 2 + target) % 2, peer(1 if target % 2 == 0 else NZ - 1, 0, 0, 0, 0)
        d = 1 if target % 2 == 0 else NZ - 1
        return send(
            rows_all.at[0, half(hr), lanes], rows_all.at[d, half(hr), lanes], z_s, z_r.at[target], to
        )

    def col_send(n, src, dst, to):
        r, lanes = pl.ds((n % 2) * HALF, HALF), mine if n < 2 else other
        return send(cols_all.at[src, r, lanes], cols_all.at[dst, r, lanes], col_s, col_r.at[n + (CHUNKS if dst == 3 else 0)], to)

    far_cols = [col_send(n, 0, 2, peer(0, 1, 0, 0, 0)) for n in range(CHUNKS)]
    forwards = [col_send(n, 2, 3, partner) for n in range(CHUNKS)]
    near_cols = send(cols_all.at[0], cols_all.at[1], col_s, col_r.at[2 * CHUNKS], partner)

    standardize(summed, mine)
    for target in range(2, 6):
        first_send(target, mine).start()
    for copy in far_cols[:2]:
        copy.start()
    back.wait_recv()
    standardize(total_in[...], other)
    for target in range(2, 6):
        first_send(target, other).start()
    near_cols.start()
    for copy in far_cols[2:]:
        copy.start()

    def step_unit(t):
        late = t - 2 * EARLY
        i = jnp.where(t < EARLY, t, jnp.where(t < 2 * EARLY, t - EARLY, EARLY + lax.div(late, 2)))
        u = jnp.where(t < EARLY, 0, jnp.where(t < 2 * EARLY, 1, lax.rem(late, 2)))
        return 2 * i, u

    def relay_send(t, way):
        return send(
            coded.at[t, way, 0],
            relay_in.at[t, way],
            x_s,
            rel_r.at[t],
            peer(0, 0, 0, 0, jnp.where(t >= DIRECT, 2, 3 if way else 1)),
        )

    def x_send(t, way, late):
        return send(
            coded.at[t, way, 1 + late],
            coded_in.at[t, way, late],
            x_s,
            x_r.at[t],
            peer(0, 0, 0, 0, 3 if way else 1),
        )

    def y_send(t, e, jj):
        i, u = step_unit(t)
        d, hr, _ = unit(i + e)
        return send(
            sum_coded.at[t, jj, pl.ds(e * TILE, TILE)],
            sum_in.at[d, 2 * (2 * u + jj) + hr],
            y_s,
            y_r.at[d],
            peer(0, u, jj, hr, 0),
        )

    def produce(t):
        i, u = step_unit(t)
        d0, hr0, _ = unit(i)
        d1, hr1, _ = unit(i + 1)

        @pl.when(jnp.logical_and(u == 0, i >= 12))
        def _():
            z_send(i).wait_recv()
            z_send(i + 1).wait_recv()

        lhs = jnp.concatenate([rows_all[d0, half(hr0), :], rows_all[d1, half(hr1), :]], axis=0)
        rhs = cols_all[pl.ds(2 * u, 2), :, :].reshape(512, SNPS)
        acc[...] = lax.dot_general(lhs, rhs, (((1,), (1,)), ((), ())), preferred_element_type=jnp.float32)
        for way in range(2):
            for e in range(2):
                coded[t, way, 0, rows(e)] = encode(acc[tile(e, 2), LANES[way]], X_SHIFT)
            relay_send(t, way).start()
        for way in range(2):
            for e in range(2):
                coded[t, way, 1, rows(e)] = encode(acc[tile(e, 3 if way else 1), LANES[1 - way]], X_SHIFT)
            x_send(t, way, 0).start()

        @pl.when(t < DIRECT)
        def _():
            for way in range(2):
                for e in range(2):
                    kept[t, way, rows(e)] = acc[tile(e, 3 if way else 1), LANES[way]]

        @pl.when(t >= DIRECT)
        def _():
            for way in range(2):
                for e in range(2):
                    coded[t, way, 2, rows(e)] = encode(acc[tile(e, 3 if way else 1), LANES[way]], X_SHIFT)
                x_send(t, way, 1).start()

        for e in range(2):
            own[t, rows(e)] = acc[tile(e, 0), :]

    def rows(e):
        return pl.ds(e * TILE, TILE)

    def tile(e, dx):
        return pl.ds(pl.multiple_of(e * HALF + lax.rem(x + dx, NX) * TILE, TILE), TILE)

    def relay(t):
        arrived(relay_in.at[t], rel_r.at[t])
        for way in range(2):
            coded[t, way, 2] = encode(kept[t, way] + decode(relay_in[t, way], X_SHIFT), X_SHIFT)
            x_send(t, way, 1).start()

    def consume(t):
        i, u = step_unit(t)
        arrived(coded_in.at[t], x_r.at[t])

        @pl.when(t >= DIRECT)
        def _():
            arrived(relay_in.at[t], rel_r.at[t])
            for way in range(2):
                own[t, :, LANES[way]] = own[t, :, LANES[way]] + decode(relay_in[t, way], X_SHIFT)

        left = own[t, :, 0:256] + decode(coded_in[t, 0, 1], X_SHIFT) + decode(coded_in[t, 1, 0], X_SHIFT)
        code = encode(left, Y_SHIFT)
        sum_coded[t, 0] = code
        for e in range(2):
            d, hr, _ = unit(i + e)
            here = jnp.logical_and(u == 0, hr == 0)

            @pl.when(here)
            def _(d=d, e=e):
                sum_in[d, 0] = code[e * TILE : (e + 1) * TILE]

            @pl.when(jnp.logical_not(here))
            def _(e=e):
                y_send(t, e, 0).start()

        right = own[t, :, 256:512] + decode(coded_in[t, 0, 0], X_SHIFT) + decode(coded_in[t, 1, 1], X_SHIFT)
        sum_coded[t, 1] = encode(right, Y_SHIFT)
        for e in range(2):
            y_send(t, e, 1).start()

    def step(t, carry):
        @pl.when(t == 0)
        def _():
            near_cols.wait_recv()

        for at, chunks in FORWARD.items():

            @pl.when(t == at)
            def _(chunks=chunks):
                for n in chunks:
                    far_cols[n].wait_recv()
                    forwards[n].start()

        @pl.when(jnp.logical_and(t >= RELAY_LAG, t < DIRECT + RELAY_LAG))
        def _():
            relay(t - RELAY_LAG)

        @pl.when(t >= SUM_LAG)
        def _():
            consume(t - SUM_LAG)

        for at, pairs in PASS_ON.items():

            @pl.when(t == at)
            def _(pairs=pairs):
                for got, target in pairs:
                    z_send(got).wait_recv()
                    z_send(target).start()

        @pl.when(t == EARLY)
        def _():
            for copy in forwards:
                copy.wait_recv()

        @pl.when(t < STEPS)
        def _():
            produce(t)

        for at, planes in FINISH.items():

            @pl.when(t == at)
            def _(planes=planes):
                for d in planes:
                    finish(d)

        return carry

    def finish(d):
        arrived(sum_in.at[d, pl.ds(1, 7)], y_r.at[d])
        for j in range(4):
            value = decode(sum_in[d, 2 * j], Y_SHIFT) + decode(sum_in[d, 2 * j + 1], Y_SHIFT)
            q = lax.rem(z + NZ - d, NZ) * 4 + lax.rem(a + j // 2, 2) * 2 + lax.rem(c + j % 2, 2)
            out_ref[q, 0] = value * (1.0 / 8192.0)

    lax.fori_loop(0, STEPS + SUM_LAG, step, 0)
    for d in LAST:
        finish(d)

    sent(sums_in, st_s.at[1])
    swap.wait_send()
    back.wait_send()
    sent(cols_all.at[pl.ds(0, 3)], col_s)
    sent(rows_all.at[pl.ds(0, 7)], z_s)
    sent(coded, x_s)
    sent(sum_coded.at[pl.ds(0, STEPS - NZ // 4)], y_s)


def body(genotypes, observed):
    f32, bf16, s16 = jnp.float32, jnp.bfloat16, jnp.int16
    dma = pltpu.SemaphoreType.DMA
    return pl.pallas_call(
        kernel,
        out_shape=jax.ShapeDtypeStruct((32, 1, TILE, ROWS), f32),
        in_specs=[pl.BlockSpec(memory_space=pl.ANY)] * 2,
        out_specs=pl.BlockSpec(memory_space=pltpu.VMEM),
        scratch_shapes=[
            pltpu.VMEM((ROWS, SNPS), f32),
            pltpu.VMEM((ROWS, SNPS), jnp.int32),
            pltpu.VMEM((2, SNPS), f32),
            pltpu.VMEM((2, 512), f32),
            pltpu.VMEM((2, 512), f32),
            pltpu.VMEM((15, 2, 512), f32),
            pltpu.VMEM((2, 512), f32),
            pltpu.VMEM((2, 512), f32),
            pltpu.VMEM((NZ, ROWS, SNPS), bf16),
            pltpu.VMEM((4, ROWS, SNPS), bf16),
            pltpu.VMEM((2 * HALF, 512), f32),
            pltpu.VMEM((STEPS, 2, 3, 2 * TILE, ROWS), s16),
            pltpu.VMEM((STEPS, 2, 2 * TILE, ROWS), s16),
            pltpu.VMEM((STEPS, 2, 2, 2 * TILE, ROWS), s16),
            pltpu.VMEM((STEPS, 2 * TILE, 512), f32),
            pltpu.VMEM((STEPS, 2, 2 * TILE, ROWS), f32),
            pltpu.VMEM((STEPS, 2, 2 * TILE, ROWS), s16),
            pltpu.VMEM((NZ, 8, TILE, ROWS), s16),
            dma((4,)),
            dma((3,)),
            dma((17,)),
            dma(()),
            dma((2 * CHUNKS + 1,)),
            dma(()),
            dma((UNITS,)),
            dma(()),
            dma((STEPS,)),
            dma((STEPS,)),
            dma(()),
            dma((NZ,)),
        ],
        compiler_params=pltpu.CompilerParams(
            collective_id=0, has_side_effects=True, vmem_limit_bytes=int(32 * 2**20)
        ),
    )(pltpu.with_memory_space_constraint(genotypes, pltpu.HBM), pltpu.with_memory_space_constraint(observed, pltpu.HBM))


def solution(mesh):
    return jax.shard_map(
        body,
        mesh=mesh,
        in_specs=(P("samp", "snp"), P("samp", "snp")),
        out_specs=P(None, "snp", None, "samp"),
        check_vma=False,
    )
```

```python
import jax
import jax.numpy as jnp
from jax import lax
from jax.experimental import pallas as pl
from jax.experimental.pallas import tpu as pltpu
from jax.sharding import PartitionSpec as P

var_floor = 0.1
MESH = pl.DeviceIdType.MESH
NZ, NX, TILE = 8, 4, 32
ROWS, SNPS = 256, 1024
HALF = 128
UNITS = 16
STEPS = UNITS
EARLY = 3
RELAY_LAG, SUM_LAG = 2, 4
X_SHIFT, Y_SHIFT = 15.0, 14.0
STEPS_PER_OCTAVE = 1024.0
DIRECT = 15
PASS_ON = {
    1: ((2, 6), (3, 7)),
    2: ((4, 8), (5, 9)),
    6: ((6, 10), (7, 11)),
    8: ((8, 12), (9, 13)),
    10: ((10, 14), (11, 15)),
}
CHUNKS = 4
FORWARD = {2: (0, 1), 3: (2, 3)}
LANES = (slice(0, 256), slice(256, 512))
FINISH = {SUM_LAG + 5: (0,), SUM_LAG + 8: (1, 7), SUM_LAG + 12: (2, 6)}
LAST = (3, 5, 4)

STATS_PEERS = sorted(
    [(dz, da, 0, 0, 0) for dz in range(NZ) for da in range(2) if (dz, da) != (0, 0)],
    key=lambda p: (-min(p[0], NZ - p[0]) - 2 * p[1], p),
)
PEERS = (
    STATS_PEERS
    + [(0, 1, 1, 0, 0)]
    + [(0, da, dc, 1, 0) for da in range(2) for dc in range(2)]
    + [(0, 0, 0, 0, dx) for dx in (2, 1, 3)]
    + [(0, 0, 1, 0, 0)]
)


def encode(value, shift):
    level = jnp.log2(jnp.abs(value)) * STEPS_PER_OCTAVE + (shift * STEPS_PER_OCTAVE + 0.5)
    level = jnp.maximum(level, 0.25).astype(jnp.int32)
    return jnp.where(value < 0.0, -level, level).astype(jnp.int16)


def decode(code, shift):
    level = code.astype(jnp.int32).astype(jnp.float32)
    size = jnp.exp2(jnp.abs(level) * (1.0 / STEPS_PER_OCTAVE) - shift)
    return jnp.clip(level, -1.0, 1.0) * size


def kernel(
    g_hbm, o_hbm, out_ref,
    g_ref, o_ref, part, part_in, pair, sums_in, total, total_in,
    rows_all, cols_all, acc, coded, relay_in, coded_in, own, kept, sum_coded, sum_in,
    load_sem, st_s, st_r, col_s, col_r, z_s, z_r, x_s, rel_r, x_r, y_s, y_r,
):
    samp = lax.axis_index("samp")
    snp = lax.axis_index("snp")
    z = lax.div(samp, 4)
    a = lax.rem(lax.div(samp, 2), 2)
    c = lax.rem(samp, 2)
    yl = lax.div(snp, NX)
    x = lax.rem(snp, NX)

    def peer(dz, da, dc, dyl, dx):
        return (
            lax.rem(z + dz, NZ) * 4 + lax.rem(a + da, 2) * 2 + lax.rem(c + dc, 2),
            lax.rem(yl + dyl, 2) * NX + lax.rem(x + dx, NX),
        )

    def send(src, dst, s_sem, r_sem, to):
        return pltpu.make_async_remote_copy(
            src_ref=src, dst_ref=dst, send_sem=s_sem, recv_sem=r_sem, device_id=to, device_id_type=MESH
        )

    def arrived(ref, sem):
        send(ref, ref, sem, sem, peer(0, 0, 1, 0, 0)).wait_recv()

    def sent(ref, sem):
        send(ref, ref, sem, sem, peer(0, 0, 1, 0, 0)).wait_send()

    loads = []
    for n in range(2):
        r = pl.ds(n * HALF, HALF)
        loads.append(pltpu.make_async_copy(g_hbm.at[r], g_ref.at[r], load_sem.at[2 * n]))
        loads.append(pltpu.make_async_copy(o_hbm.at[r], o_ref.at[r], load_sem.at[2 * n + 1]))
    for copy in loads:
        copy.start()
    barrier = pltpu.get_barrier_semaphore()
    for p in PEERS:
        pl.semaphore_signal(barrier, inc=1, device_id=peer(*p), device_id_type=MESH)
    def count(i, carry):
        alt, call = carry
        present = o_ref[pl.ds(i * 8, 8), :].astype(jnp.float32)
        return alt + present * g_ref[pl.ds(i * 8, 8), :], call + present

    zero = jnp.zeros((8, SNPS), jnp.float32)
    counts = (zero, zero)
    for n in range(2):
        for copy in loads[2 * n : 2 * n + 2]:
            copy.wait()
        counts = lax.fori_loop(n * HALF // 8, (n + 1) * HALF // 8, count, counts, unroll=8)
    alt8, call8 = counts
    part[0:1, :] = jnp.sum(alt8, axis=0, keepdims=True)
    part[1:2, :] = jnp.sum(call8, axis=0, keepdims=True)
    pl.semaphore_wait(barrier, len(PEERS))

    partner = peer(0, 0, 1, 0, 0)
    mine = pl.ds(pl.multiple_of(c * 512, 512), 512)
    other = pl.ds(pl.multiple_of((1 - c) * 512, 512), 512)
    swap = send(part.at[:, other], part_in, st_s.at[0], st_r.at[0], partner)
    swap.start()
    swap.wait_recv()
    pair[...] = part[:, mine] + part_in[...]
    spread = []
    for n, p in enumerate(STATS_PEERS):
        copy = send(pair, sums_in.at[n], st_s.at[1], st_r.at[1 + n], peer(*p))
        copy.start()
        spread.append(copy)
    summed = pair[...]
    for n, copy in reversed(list(enumerate(spread))):
        copy.wait_recv()
        summed = summed + sums_in[n]
    total[...] = summed
    back = send(total, total_in, st_s.at[2], st_r.at[16], partner)
    back.start()

    def standardize(stats, lanes):
        frequency = stats[0:1, :] / (2.0 * jnp.maximum(stats[1:2, :], 1.0))
        variance = jnp.maximum(2.0 * frequency * (1.0 - frequency), var_floor)
        twice = 2.0 * frequency
        scale = lax.rsqrt(variance)

        def rows_of(i, carry):
            r = pl.ds(i * 32, 32)
            value = o_ref[r, lanes].astype(jnp.float32) * (g_ref[r, lanes] - twice) * scale
            value = value.astype(jnp.bfloat16)
            rows_all[0, r, lanes] = value
            cols_all[0, r, lanes] = value
            return carry

        lax.fori_loop(0, ROWS // 32, rows_of, 0, unroll=True)

    def unit(i):
        m = i - 2
        r = lax.div(m, 4)
        back_way = lax.rem(m, 2)
        hr = lax.rem(lax.div(lax.rem(m, 4), 2) + back_way, 2)
        d = jnp.where(back_way == 1, 7 - r, 1 + r)
        d = jnp.where(i < 2, 0, jnp.where(i >= 14, 4, d))
        hr = jnp.where(i < 2, i, jnp.where(i >= 14, i - 14, hr))
        back_way = jnp.where(i >= 14, i - 14, back_way)
        return d, hr, back_way

    def half(hr):
        return pl.ds(pl.multiple_of(lax.rem(yl + hr, 2) * HALF, HALF), HALF)

    def z_send(target):
        d, hr, back_way = unit(target)
        src = jnp.where(back_way == 1, lax.rem(d + 1, NZ), d - 1)
        to = peer(jnp.where(back_way == 1, NZ - 1, 1), 0, 0, 0, 0)
        return send(rows_all.at[src, half(hr)], rows_all.at[d, half(hr)], z_s, z_r.at[target], to)

    def first_send(target, lanes):
        hr, to = ((target - 2) // 2 + target) % 2, peer(1 if target % 2 == 0 else NZ - 1, 0, 0, 0, 0)
        d = 1 if target % 2 == 0 else NZ - 1
        return send(
            rows_all.at[0, half(hr), lanes], rows_all.at[d, half(hr), lanes], z_s, z_r.at[target], to
        )

    def col_send(n, src, dst, to):
        r, lanes = pl.ds((n % 2) * HALF, HALF), mine if n < 2 else other
        return send(cols_all.at[src, r, lanes], cols_all.at[dst, r, lanes], col_s, col_r.at[n + (CHUNKS if dst == 3 else 0)], to)

    far_cols = [col_send(n, 0, 2, peer(0, 1, 0, 0, 0)) for n in range(CHUNKS)]
    forwards = [col_send(n, 2, 3, partner) for n in range(CHUNKS)]
    near_cols = send(cols_all.at[0], cols_all.at[1], col_s, col_r.at[2 * CHUNKS], partner)

    standardize(summed, mine)
    for copy in far_cols[:2]:
        copy.start()
    for target in range(2, 6):
        first_send(target, mine).start()
    back.wait_recv()
    standardize(total_in[...], other)
    near_cols.start()
    for copy in far_cols[2:]:
        copy.start()
    for target in range(2, 6):
        first_send(target, other).start()

    def step_unit(t):
        late = t - 2 * EARLY
        i = jnp.where(t < EARLY, t, jnp.where(t < 2 * EARLY, t - EARLY, EARLY + lax.div(late, 2)))
        u = jnp.where(t < EARLY, 0, jnp.where(t < 2 * EARLY, 1, lax.rem(late, 2)))
        return 2 * i, u

    def relay_send(t, way):
        return send(
            coded.at[t, way, 0],
            relay_in.at[t, way],
            x_s,
            rel_r.at[t],
            peer(0, 0, 0, 0, jnp.where(t >= DIRECT, 2, 3 if way else 1)),
        )

    def x_send(t, way, late):
        return send(
            coded.at[t, way, 1 + late],
            coded_in.at[t, way, late],
            x_s,
            x_r.at[t],
            peer(0, 0, 0, 0, 3 if way else 1),
        )

    def y_send(t, e, jj):
        i, u = step_unit(t)
        d, hr, _ = unit(i + e)
        return send(
            sum_coded.at[t, jj, pl.ds(e * TILE, TILE)],
            sum_in.at[d, 2 * (2 * u + jj) + hr],
            y_s,
            y_r.at[d],
            peer(0, u, jj, hr, 0),
        )

    def produce(t):
        i, u = step_unit(t)
        d0, hr0, _ = unit(i)
        d1, hr1, _ = unit(i + 1)

        @pl.when(jnp.logical_and(u == 0, i >= 12))
        def _():
            z_send(i).wait_recv()
            z_send(i + 1).wait_recv()

        lhs = jnp.concatenate([rows_all[d0, half(hr0), :], rows_all[d1, half(hr1), :]], axis=0)
        rhs = cols_all[pl.ds(2 * u, 2), :, :].reshape(512, SNPS)
        acc[...] = lax.dot_general(lhs, rhs, (((1,), (1,)), ((), ())), preferred_element_type=jnp.float32)
        for way in range(2):
            for e in range(2):
                coded[t, way, 0, rows(e)] = encode(acc[tile(e, 2), LANES[way]], X_SHIFT)
            relay_send(t, way).start()
        for way in range(2):
            for e in range(2):
                coded[t, way, 1, rows(e)] = encode(acc[tile(e, 3 if way else 1), LANES[1 - way]], X_SHIFT)
            x_send(t, way, 0).start()

        @pl.when(t < DIRECT)
        def _():
            for way in range(2):
                for e in range(2):
                    kept[t, way, rows(e)] = acc[tile(e, 3 if way else 1), LANES[way]]

        @pl.when(t >= DIRECT)
        def _():
            for way in range(2):
                for e in range(2):
                    coded[t, way, 2, rows(e)] = encode(acc[tile(e, 3 if way else 1), LANES[way]], X_SHIFT)
                x_send(t, way, 1).start()

        for e in range(2):
            own[t, rows(e)] = acc[tile(e, 0), :]

    def rows(e):
        return pl.ds(e * TILE, TILE)

    def tile(e, dx):
        return pl.ds(pl.multiple_of(e * HALF + lax.rem(x + dx, NX) * TILE, TILE), TILE)

    def relay(t):
        arrived(relay_in.at[t], rel_r.at[t])
        for way in range(2):
            coded[t, way, 2] = encode(kept[t, way] + decode(relay_in[t, way], X_SHIFT), X_SHIFT)
            x_send(t, way, 1).start()

    def consume(t):
        i, u = step_unit(t)
        arrived(coded_in.at[t], x_r.at[t])

        @pl.when(t >= DIRECT)
        def _():
            arrived(relay_in.at[t], rel_r.at[t])
            for way in range(2):
                own[t, :, LANES[way]] = own[t, :, LANES[way]] + decode(relay_in[t, way], X_SHIFT)

        left = own[t, :, 0:256] + decode(coded_in[t, 0, 1], X_SHIFT) + decode(coded_in[t, 1, 0], X_SHIFT)
        code = encode(left, Y_SHIFT)
        sum_coded[t, 0] = code
        for e in range(2):
            d, hr, _ = unit(i + e)
            here = jnp.logical_and(u == 0, hr == 0)

            @pl.when(here)
            def _(d=d, e=e):
                sum_in[d, 0] = code[e * TILE : (e + 1) * TILE]

            @pl.when(jnp.logical_not(here))
            def _(e=e):
                y_send(t, e, 0).start()

        right = own[t, :, 256:512] + decode(coded_in[t, 0, 0], X_SHIFT) + decode(coded_in[t, 1, 1], X_SHIFT)
        sum_coded[t, 1] = encode(right, Y_SHIFT)
        for e in range(2):
            y_send(t, e, 1).start()

    def step(t, carry):
        @pl.when(t == 0)
        def _():
            near_cols.wait_recv()

        for at, chunks in FORWARD.items():

            @pl.when(t == at)
            def _(chunks=chunks):
                for n in chunks:
                    far_cols[n].wait_recv()
                    forwards[n].start()

        @pl.when(jnp.logical_and(t >= RELAY_LAG, t < DIRECT + RELAY_LAG))
        def _():
            relay(t - RELAY_LAG)

        @pl.when(t >= SUM_LAG)
        def _():
            consume(t - SUM_LAG)

        for at, pairs in PASS_ON.items():

            @pl.when(t == at)
            def _(pairs=pairs):
                for got, target in pairs:
                    z_send(got).wait_recv()
                    z_send(target).start()

        @pl.when(t == EARLY)
        def _():
            for copy in forwards:
                copy.wait_recv()

        @pl.when(t < STEPS)
        def _():
            produce(t)

        for at, planes in FINISH.items():

            @pl.when(t == at)
            def _(planes=planes):
                for d in planes:
                    finish(d)

        return carry

    def finish(d):
        arrived(sum_in.at[d, pl.ds(1, 7)], y_r.at[d])
        for j in range(4):
            value = decode(sum_in[d, 2 * j], Y_SHIFT) + decode(sum_in[d, 2 * j + 1], Y_SHIFT)
            q = lax.rem(z + NZ - d, NZ) * 4 + lax.rem(a + j // 2, 2) * 2 + lax.rem(c + j % 2, 2)
            out_ref[q, 0] = value * (1.0 / 8192.0)

    lax.fori_loop(0, STEPS + SUM_LAG, step, 0)
    for d in LAST:
        finish(d)

    sent(sums_in, st_s.at[1])
    swap.wait_send()
    back.wait_send()
    sent(cols_all.at[pl.ds(0, 3)], col_s)
    sent(rows_all.at[pl.ds(0, 7)], z_s)
    sent(coded, x_s)
    sent(sum_coded.at[pl.ds(0, STEPS - NZ // 4)], y_s)


def body(genotypes, observed):
    f32, bf16, s16 = jnp.float32, jnp.bfloat16, jnp.int16
    dma = pltpu.SemaphoreType.DMA
    return pl.pallas_call(
        kernel,
        out_shape=jax.ShapeDtypeStruct((32, 1, TILE, ROWS), f32),
        in_specs=[pl.BlockSpec(memory_space=pl.ANY)] * 2,
        out_specs=pl.BlockSpec(memory_space=pltpu.VMEM),
        scratch_shapes=[
            pltpu.VMEM((ROWS, SNPS), f32),
            pltpu.VMEM((ROWS, SNPS), jnp.int32),
            pltpu.VMEM((2, SNPS), f32),
            pltpu.VMEM((2, 512), f32),
            pltpu.VMEM((2, 512), f32),
            pltpu.VMEM((15, 2, 512), f32),
            pltpu.VMEM((2, 512), f32),
            pltpu.VMEM((2, 512), f32),
            pltpu.VMEM((NZ, ROWS, SNPS), bf16),
            pltpu.VMEM((4, ROWS, SNPS), bf16),
            pltpu.VMEM((2 * HALF, 512), f32),
            pltpu.VMEM((STEPS, 2, 3, 2 * TILE, ROWS), s16),
            pltpu.VMEM((STEPS, 2, 2 * TILE, ROWS), s16),
            pltpu.VMEM((STEPS, 2, 2, 2 * TILE, ROWS), s16),
            pltpu.VMEM((STEPS, 2 * TILE, 512), f32),
            pltpu.VMEM((STEPS, 2, 2 * TILE, ROWS), f32),
            pltpu.VMEM((STEPS, 2, 2 * TILE, ROWS), s16),
            pltpu.VMEM((NZ, 8, TILE, ROWS), s16),
            dma((4,)),
            dma((3,)),
            dma((17,)),
            dma(()),
            dma((2 * CHUNKS + 1,)),
            dma(()),
            dma((UNITS,)),
            dma(()),
            dma((STEPS,)),
            dma((STEPS,)),
            dma(()),
            dma((NZ,)),
        ],
        compiler_params=pltpu.CompilerParams(
            collective_id=0, has_side_effects=True, vmem_limit_bytes=int(32 * 2**20)
        ),
    )(pltpu.with_memory_space_constraint(genotypes, pltpu.HBM), pltpu.with_memory_space_constraint(observed, pltpu.HBM))


def solution(mesh):
    return jax.shard_map(
        body,
        mesh=mesh,
        in_specs=(P("samp", "snp"), P("samp", "snp")),
        out_specs=P(None, "snp", None, "samp"),
        check_vma=False,
    )
```
